256 devices in a mesh: row: 16 (over z, core), col: 16 (over x, y).
Axes of the slice: x: 4, y: 4, z: 8, core: 2. Of those that a mesh axis runs over, the one named last changes fastest.
Arguments:
- images: bfloat16 [4096, 12, 12, 272], P(('row', 'col')), may hold values from -20 to 20
- expand_weight: bfloat16 [2, 272, 1632], replicated, may hold values from -0.375 to 0.375
- depth_kernel: float32 [2, 25, 1632], replicated, may hold values from -1.25 to 1.25
- squeeze_weight: float32 [2, 1632, 68], replicated, may hold values from -0.15625 to 0.15625
- squeeze_bias: float32 [2, 68], replicated, may hold values from -3 to 3
- excite_weight: float32 [2, 68, 1632], replicated, may hold values from -0.75 to 0.75
- excite_bias: float32 [2, 1632], replicated, may hold values from -4 to 4
- project_weight: bfloat16 [2, 1632, 272], replicated, may hold values from -0.15625 to 0.15625
- mid_gain: float32 [2, 2, 1632], replicated, may hold values from 0.5 to 1.5
- mid_bias: float32 [2, 2, 1632], replicated, may hold values from -3 to 3
- out_gain: float32 [2, 272], replicated, may hold values from 0.5 to 1.5
- out_bias: float32 [2, 272], replicated, may hold values from -3 to 3
- mid_mean: float32 [2, 2, 1632], replicated, may hold values from -4 to 4
- mid_var: float32 [2, 2, 1632], replicated, may hold values from 0.05 to 20
- out_mean: float32 [2, 272], replicated, may hold values from -4 to 4
- out_var: float32 [2, 272], replicated, may hold values from 0.05 to 20
Outputs:
- block_output: bfloat16 [4096, 12, 12, 272], P(('row', 'col'))
- mid_mean_new: float32 [2, 2, 1632], replicated
- mid_var_new: float32 [2, 2, 1632], replicated
- out_mean_new: float32 [2, 272], replicated
- out_var_new: float32 [2, 272], replicated
The draws below stay inside these ranges and needn't reach their ends.
All inputs are finite; a program needn't handle non-finite values.
Results may differ from the reference program's by a relative error of at most 0.0049.
The reference program's roundings to bfloat16 on the way (of `active` and `scaled`) count: a program that leaves them out, or rounds other values in their place, can miss the bound.
Values sent between devices are 32-bit elements; how exact they have to be, the bound alone decides.
No kernel may reach another device: no remote copies, remote signals or barrier semaphores. Data moves between devices by JAX's collectives and lax.ppermute only.
A program may use at most 128 MiB of HBM per device.

```python
import math
import jax
import jax.numpy as jnp
from jax import lax

OUT = 272
MID = 1632
SQZ = 68
KERN = 5
SIDE = 12
LAYERS = 2
BATCH = 4096


def draw_images(key, part):
    subkeys = jax.random.split(jax.random.fold_in(key, 11), 2)
    rising = 1.0 + 2.0 * jnp.arange(BATCH, dtype=jnp.float32) / max(BATCH - 1, 1)
    offset = 0.5 * jax.random.truncated_normal(subkeys[0], -4.0, 4.0, (OUT,), jnp.float32)
    noise_draw = jax.random.truncated_normal(subkeys[1], -4.0, 4.0, (BATCH, SIDE, SIDE, OUT), jnp.float32)
    return (noise_draw * rising[:, None, None, None] + offset).astype(jnp.bfloat16)


def scatter_about(key, extent, deviation, most, held_as=jnp.bfloat16):
    array = jax.random.normal(key, extent, jnp.float32) * deviation
    return jnp.minimum(jnp.maximum(array, -most), most).astype(held_as)


def setup_inputs(seed: int = 0) -> dict:
    streams_of = jax.random.split(jax.random.key(seed), 17)
    return {
        "images": draw_images(jax.random.fold_in(streams_of[16], 71), 0),
        "expand_weight": scatter_about(streams_of[1], (LAYERS, OUT, MID), OUT ** -0.5, 0.375),
        "depth_kernel": scatter_about(streams_of[2], (LAYERS, KERN * KERN, MID), (KERN * KERN) ** -0.5, 1.25, jnp.float32),
        "squeeze_weight": scatter_about(streams_of[3], (LAYERS, MID, SQZ), MID ** -0.5, 0.15625, jnp.float32),
        "squeeze_bias": scatter_about(streams_of[4], (LAYERS, SQZ), 0.5, 3.0, jnp.float32),
        "excite_weight": scatter_about(streams_of[5], (LAYERS, SQZ, MID), SQZ ** -0.5, 0.75, jnp.float32),
        "excite_bias": scatter_about(streams_of[6], (LAYERS, MID), 1.0, 4.0, jnp.float32),
        "project_weight": scatter_about(streams_of[7], (LAYERS, MID, OUT), MID ** -0.5, 0.15625),
        "mid_gain": jnp.clip(1.0 + 0.1 * jax.random.normal(streams_of[8], (LAYERS, 2, MID), jnp.float32), 0.5, 1.5),
        "mid_bias": scatter_about(streams_of[9], (LAYERS, 2, MID), 0.5, 3.0, jnp.float32),
        "out_gain": jnp.clip(1.0 + 0.1 * jax.random.normal(streams_of[10], (LAYERS, OUT), jnp.float32), 0.5, 1.5),
        "out_bias": scatter_about(streams_of[11], (LAYERS, OUT), 0.5, 3.0, jnp.float32),
        "mid_mean": scatter_about(streams_of[12], (LAYERS, 2, MID), 1.0, 4.0, jnp.float32),
        "mid_var": jnp.clip(jnp.exp(jax.random.uniform(streams_of[13], (LAYERS, 2, MID), jnp.float32, math.log(0.05), math.log(20.0))), 0.05, 20.0),
        "out_mean": scatter_about(streams_of[14], (LAYERS, OUT), 1.0, 4.0, jnp.float32),
        "out_var": jnp.clip(jnp.exp(jax.random.uniform(streams_of[15], (LAYERS, OUT), jnp.float32, math.log(0.05), math.log(20.0))), 0.05, 20.0),
    }


EPSILON = 0.001
RATIO_MAX = 3.0
SHIFT_MAX = 5.0
MOMENTUM = 0.01

def coefficients(first_sum, second_sum, row_count, run_mean, run_var, gain, bias):
    offset = first_sum / row_count
    batch_var = second_sum / row_count - offset * offset
    batch_mean = run_mean + offset
    batch_sigma = jnp.sqrt(batch_var + EPSILON)
    run_sigma = jnp.sqrt(run_var + EPSILON)
    scale_ratio = jnp.clip(batch_sigma / run_sigma, 1.0 / RATIO_MAX, RATIO_MAX)
    shift_clip = jnp.clip(offset / run_sigma, -SHIFT_MAX, SHIFT_MAX)
    gain_scale = gain * scale_ratio / batch_sigma
    gain_shift = bias + gain * shift_clip - batch_mean * gain_scale
    new_mean = run_mean + MOMENTUM * offset
    new_var = run_var + MOMENTUM * (batch_var - run_var)
    return (gain_scale, gain_shift, new_mean, new_var)

def moments(values, run_mean):
    centered = values - run_mean
    return (lax.optimization_barrier(jnp.sum(centered, axis=(0, 1, 2))), lax.optimization_barrier(jnp.sum(centered * centered, axis=(0, 1, 2))))

def project_rows(images, matrix):
    leading = images.shape[:3]
    flat_rows = images.reshape(-1, images.shape[3])
    product = jnp.dot(flat_rows, matrix, preferred_element_type=jnp.float32)
    return product.reshape(leading + (matrix.shape[1],))

def depthwise(active, kernel):
    reach = KERN // 2
    side_len = active.shape[1]
    padded = jnp.pad(active, ((0, 0), (reach, reach), (reach, reach), (0, 0)))
    running_total = jnp.zeros(active.shape, jnp.float32)
    for row_step in range(KERN):
        for col_step in range(KERN):
            window = padded[:, row_step:row_step + side_len, col_step:col_step + side_len, :]
            running_total = running_total + window * kernel[row_step * KERN + col_step]
    return running_total

def excite(lifted, reduce_w, reduce_b, grow_w, grow_b):
    pooled = lax.optimization_barrier(jnp.mean(lifted, axis=(1, 2)))
    squeezed = jax.nn.silu(jnp.dot(pooled, reduce_w, precision=lax.Precision.HIGHEST) + reduce_b)
    se_gate = jax.nn.sigmoid(jnp.dot(squeezed, grow_w, precision=lax.Precision.HIGHEST) + grow_b)
    return (lifted * se_gate[:, None, None, :]).astype(jnp.bfloat16)

def through(group, params, scales, norm_depth):
    expand_w, kernel, reduce_w, reduce_b, grow_w, grow_b, project_w = params
    expanded = project_rows(group, expand_w)
    if norm_depth == 0:
        return expanded
    active = jax.nn.silu(expanded * scales[0][0] + scales[0][1]).astype(jnp.bfloat16)
    spread = depthwise(active, kernel)
    if norm_depth == 1:
        return spread
    lifted = jax.nn.silu(spread * scales[1][0] + scales[1][1])
    scaled = excite(lifted, reduce_w, reduce_b, grow_w, grow_b)
    projected = project_rows(scaled, project_w)
    if norm_depth == 2:
        return projected
    return (group.astype(jnp.float32) + projected * scales[2][0] + scales[2][1]).astype(jnp.bfloat16)

def reference(images, expand_weight, depth_kernel, squeeze_weight, squeeze_bias, excite_weight, excite_bias, project_weight, mid_gain, mid_bias, out_gain, out_bias, mid_mean, mid_var, out_mean, out_var):
    row_count = float(BATCH * SIDE * SIDE)
    block = math.gcd(BATCH, 32)
    current = images
    mean_layers, var_layers, out_means, out_vars = ([], [], [], [])
    for layer_index in range(LAYERS):
        params = (expand_weight[layer_index], depth_kernel[layer_index], squeeze_weight[layer_index], squeeze_bias[layer_index], excite_weight[layer_index], excite_bias[layer_index], project_weight[layer_index])
        norm_stats = [(mid_mean[layer_index, 0], mid_var[layer_index, 0], mid_gain[layer_index, 0], mid_bias[layer_index, 0]), (mid_mean[layer_index, 1], mid_var[layer_index, 1], mid_gain[layer_index, 1], mid_bias[layer_index, 1]), (out_mean[layer_index], out_var[layer_index], out_gain[layer_index], out_bias[layer_index])]
        grouped = current.reshape((BATCH // block, block) + current.shape[1:])
        scales = []
        new_stats = []
        for norm_depth in range(3):
            run_mean, run_var, gain, bias = norm_stats[norm_depth]
            first_parts, second_parts = lax.map(lambda group: moments(through(group, params, scales, norm_depth), run_mean), grouped)
            gain_scale, gain_shift, new_mean, new_var = coefficients(lax.optimization_barrier(jnp.sum(first_parts, axis=0)), lax.optimization_barrier(jnp.sum(second_parts, axis=0)), row_count, run_mean, run_var, gain, bias)
            scales.append((gain_scale, gain_shift))
            new_stats.append((new_mean, new_var))
        current = lax.map(lambda group: through(group, params, scales, 3), grouped).reshape(current.shape)
        mean_layers.append(jnp.stack([new_stats[0][0], new_stats[1][0]]))
        var_layers.append(jnp.stack([new_stats[0][1], new_stats[1][1]]))
        out_means.append(new_stats[2][0])
        out_vars.append(new_stats[2][1])
    return (current, jnp.stack(mean_layers), jnp.stack(var_layers), jnp.stack(out_means), jnp.stack(out_vars))
```

```python
import functools
import jax
import jax.numpy as jnp
from jax import lax
from jax.experimental import pallas as pl
from jax.experimental.pallas import tpu as pltpu
from jax.sharding import PartitionSpec as P

KERN = 5
LAYERS = 2
EPSILON = 0.001
RATIO_MAX = 3.0
SHIFT_MAX = 5.0
MOMENTUM = 0.01
LANE = 128
WIDE = 256


def coefficients(received, row_count, run_mean, run_var, gain, bias):
    sums = jnp.sum(received, axis=0)
    offset = sums[0:1] / row_count
    batch_var = sums[1:2] / row_count - offset * offset
    batch_mean = run_mean + offset
    batch_sigma = jnp.sqrt(batch_var + EPSILON)
    run_sigma = jnp.sqrt(run_var + EPSILON)
    scale_ratio = jnp.clip(batch_sigma / run_sigma, 1.0 / RATIO_MAX, RATIO_MAX)
    shift_clip = jnp.clip(offset / run_sigma, -SHIFT_MAX, SHIFT_MAX)
    gain_scale = gain * scale_ratio / batch_sigma
    gain_shift = bias + gain * shift_clip - batch_mean * gain_scale
    new_mean = run_mean + MOMENTUM * offset
    new_var = run_var + MOMENTUM * (batch_var - run_var)
    return gain_scale, gain_shift, new_mean, new_var


def half_silu(half):
    return half + half * jnp.tanh(half)


def fold_rows(block):
    return jnp.sum(block.reshape(block.shape[0] // 8, 8, block.shape[1]), axis=0)


def store_stats(stat_ref, first, second):
    members = stat_ref.shape[0]
    pair = jnp.concatenate(
        [jnp.sum(first, axis=0, keepdims=True), jnp.sum(second, axis=0, keepdims=True)], axis=0
    )
    stat_ref[...] = jnp.broadcast_to(pair[None], (members,) + pair.shape)


def expand_moments(x_ref, w_ref, mean, stat_ref, chunk):
    rows = x_ref.shape[0]
    weight = w_ref[0]

    def step(i, carry):
        first, second = carry
        start = pl.multiple_of(i * chunk, chunk)
        values = jnp.dot(x_ref[pl.ds(start, chunk), :], weight, preferred_element_type=jnp.float32)
        centered = values - mean
        return first + fold_rows(centered), second + fold_rows(centered * centered)

    zero = jnp.zeros((8, weight.shape[1]), jnp.float32)
    first, second = lax.fori_loop(0, rows // chunk, step, (zero, zero))
    store_stats(stat_ref, first, second)


def moments_kernel(x_ref, w_ref, mean_ref, stat_ref, *, chunk):
    expand_moments(x_ref, w_ref, mean_ref[0, 0:1], stat_ref, chunk)


def moments_call(x, expand_weight, mid_mean, layer, members):
    rows, out = x.shape
    mid = expand_weight.shape[2]
    steps = pl.cdiv(mid, WIDE)
    return pl.pallas_call(
        functools.partial(moments_kernel, chunk=rows // 6),
        grid=(steps,),
        in_specs=[
            pl.BlockSpec((rows, out), lambda j: (0, 0)),
            pl.BlockSpec((1, out, WIDE), lambda j: (layer, 0, j)),
            pl.BlockSpec((1, 2, WIDE), lambda j: (layer, 0, j)),
        ],
        out_specs=pl.BlockSpec((members, 2, WIDE), lambda j: (0, 0, j)),
        out_shape=jax.ShapeDtypeStruct((members, 2, mid), jnp.float32),
        name="expand_moments",
    )(x, expand_weight, mid_mean)


def depth_kernel_body(
    x_ref, w_ref, dk_ref, recv_ref, mean_ref, var_ref, gain_ref, bias_ref, mean2_ref,
    spread_ref, stat_ref, new_ref, act_ref, *, row_count, side, chunk,
):
    j = pl.program_id(0)
    rows = x_ref.shape[0]
    reach = KERN // 2

    @pl.when(j % 2 == 0)
    def _():
        scale, shift, new_mean, new_var = coefficients(
            recv_ref[...], row_count, mean_ref[0, 0:1], var_ref[0, 0:1], gain_ref[0, 0:1], bias_ref[0, 0:1]
        )
        new_ref[...] = jnp.concatenate([new_mean, new_var], axis=0)
        scale = 0.5 * scale
        shift = 0.5 * shift
        weight = w_ref[0]
        cells = chunk // 16

        def step(i, carry):
            start = pl.multiple_of(i * chunk, chunk)
            values = jnp.dot(x_ref[pl.ds(start, chunk), :], weight, preferred_element_type=jnp.float32)
            active = half_silu(values * scale + shift).astype(jnp.bfloat16).astype(jnp.float32)
            active = active.reshape(cells, 2, 8, WIDE)
            at = pl.multiple_of(i * cells, cells)
            for s in range(2):
                for b in range(2):
                    act_ref[s, b, pl.ds(at, cells)] = active[:, b, :, s * LANE : (s + 1) * LANE]
            return carry

        lax.fori_loop(0, rows // chunk, step, 0)

    mean2 = mean2_ref[0, 1:2]
    s = j % 2

    def half(b, carry):
        first, second = carry
        for h in range(side):
            acc = [None] * side
            for i in range(KERN):
                r = h + i - reach
                if r < 0 or r >= side:
                    continue
                line = [act_ref[s, b, r * side + w] for w in range(side)]
                for k in range(KERN):
                    tap = dk_ref[0, i * KERN + k : i * KERN + k + 1, :]
                    tap = jnp.broadcast_to(tap, (8, LANE))
                    for w in range(side):
                        p = w + k - reach
                        if p < 0 or p >= side:
                            continue
                        term = line[p] * tap
                        acc[w] = term if acc[w] is None else acc[w] + term
            for w in range(side):
                spread_ref[h * side + w, b] = acc[w]
                centered = acc[w] - mean2
                first = first + centered
                second = second + centered * centered
        return first, second

    zero = jnp.zeros((8, LANE), jnp.float32)
    first, second = lax.fori_loop(0, 2, half, (zero, zero))
    store_stats(stat_ref, first, second)


def depth_call(x, expand_weight, depth_kernel, received, mid_mean, mid_var, mid_gain, mid_bias, layer, side, row_count):
    rows, out = x.shape
    mid = expand_weight.shape[2]
    members = received.shape[0]
    cells = side * side
    steps = pl.cdiv(mid, LANE)
    pair = pl.BlockSpec((1, 2, WIDE), lambda j: (layer, 0, j // 2))
    return pl.pallas_call(
        functools.partial(depth_kernel_body, row_count=row_count, side=side, chunk=rows // 12),
        grid=(steps,),
        in_specs=[
            pl.BlockSpec((rows, out), lambda j: (0, 0)),
            pl.BlockSpec((1, out, WIDE), lambda j: (layer, 0, j // 2)),
            pl.BlockSpec((1, KERN * KERN, LANE), lambda j: (layer, 0, j)),
            pl.BlockSpec((members, 2, WIDE), lambda j: (0, 0, j // 2)),
            pair, pair, pair, pair,
            pl.BlockSpec((1, 2, LANE), lambda j: (layer, 0, j)),
        ],
        out_specs=[
            pl.BlockSpec((cells, 2, 8, LANE), lambda j: (0, 0, 0, j)),
            pl.BlockSpec((members, 2, LANE), lambda j: (0, 0, j)),
            pl.BlockSpec((2, WIDE), lambda j: (0, j // 2)),
        ],
        out_shape=[
            jax.ShapeDtypeStruct((cells, 2, 8, mid), jnp.float32),
            jax.ShapeDtypeStruct((members, 2, mid), jnp.float32),
            jax.ShapeDtypeStruct((2, mid), jnp.float32),
        ],
        scratch_shapes=[pltpu.VMEM((2, 2, cells, 8, LANE), jnp.float32)],
        name="depthwise",
    )(x, expand_weight, depth_kernel, received, mid_mean, mid_var, mid_gain, mid_bias, mid_mean)


def lift_kernel(
    spread_ref, recv_ref, mean_ref, var_ref, gain_ref, bias_ref,
    w1_ref, b1_ref, w2_ref, b2_ref, wp_ref, mean3_ref,
    proj_ref, stat_ref, new_ref,
    lift_ref, pool_ref, gate_ref, scaled_ref, sum_ref, *, row_count, blocks, mid, layer, parts,
):
    j = pl.program_id(0)
    cells = lift_ref.shape[1]
    group = cells // parts

    @pl.when(j < blocks)
    def _():
        scale, shift, new_mean, new_var = coefficients(
            recv_ref[...], row_count, mean_ref[0, 1:2], var_ref[0, 1:2], gain_ref[0, 1:2], bias_ref[0, 1:2]
        )
        new_ref[...] = jnp.concatenate([new_mean, new_var], axis=0)
        scale = 0.5 * scale
        shift = 0.5 * shift

        def step(i, pooled):
            at = pl.multiple_of(i * 4, 4)
            values = spread_ref[pl.ds(at, 4)]
            lifted = half_silu(values * scale + shift)
            lift_ref[j, pl.ds(at, 4)] = lifted
            return pooled + jnp.sum(lifted, axis=0)

        pooled = lax.fori_loop(0, cells // 4, step, jnp.zeros((2, 8, WIDE), jnp.float32))
        pool_ref[j] = (pooled * (1.0 / cells)).reshape(16, WIDE)

    @pl.when(j == blocks)
    def _():
        last = mid - (blocks - 1) * WIDE
        squeezed = b1_ref[layer : layer + 1, :] + jnp.zeros((16, b1_ref.shape[1]), jnp.float32)
        for k in range(blocks):
            size = WIDE if k < blocks - 1 else last
            squeezed = squeezed + jnp.dot(
                pool_ref[k, :, :size], w1_ref[0, k * WIDE : k * WIDE + size, :],
                precision=lax.Precision.HIGHEST, preferred_element_type=jnp.float32,
            )
        squeezed = half_silu(0.5 * squeezed)
        for k in range(blocks):
            size = WIDE if k < blocks - 1 else last
            grown = jnp.dot(
                squeezed, w2_ref[0, :, k * WIDE : k * WIDE + size],
                precision=lax.Precision.HIGHEST, preferred_element_type=jnp.float32,
            ) + b2_ref[layer : layer + 1, k * WIDE : k * WIDE + size]
            gate_ref[k, :, :, :size] = jax.nn.sigmoid(grown).reshape(2, 8, size)

    @pl.when(j >= blocks)
    def _():
        part = j - blocks
        base = pl.multiple_of(part * group, group)
        last = mid - (blocks - 1) * WIDE
        for k in range(blocks):
            size = WIDE if k < blocks - 1 else last
            gate = gate_ref[k, :, :, :size]

            def step(i, carry):
                at = pl.multiple_of(i * 4, 4)
                lifted = lift_ref[k, pl.ds(base + at, 4), :, :, :size]
                scaled = (lifted * gate).reshape(64, size).astype(jnp.bfloat16)
                scaled_ref[pl.ds(pl.multiple_of(i * 64, 64), 64), k * WIDE : k * WIDE + size] = scaled
                return carry

            lax.fori_loop(0, group // 4, step, 0)
        projected = jnp.dot(scaled_ref[...], wp_ref[0], preferred_element_type=jnp.float32)
        proj_ref[...] = projected
        centered = projected - mean3_ref[layer : layer + 1, :]
        first = fold_rows(centered)
        second = fold_rows(centered * centered)

        @pl.when(part == 0)
        def _():
            sum_ref[0] = first
            sum_ref[1] = second

        @pl.when(part > 0)
        def _():
            sum_ref[0] += first
            sum_ref[1] += second

        @pl.when(part == parts - 1)
        def _():
            store_stats(stat_ref, sum_ref[0], sum_ref[1])


def lift_call(
    spread, received, mid_mean, mid_var, mid_gain, mid_bias,
    squeeze_weight, squeeze_bias, excite_weight, excite_bias, project_weight, out_mean, layer, row_count,
):
    cells, _, _, mid = spread.shape
    members = received.shape[0]
    out = project_weight.shape[2]
    squeeze = squeeze_weight.shape[2]
    blocks = pl.cdiv(mid, WIDE)
    parts = 3
    rows = cells * 16
    here = lambda j: jnp.minimum(j, blocks - 1)
    pair = pl.BlockSpec((1, 2, WIDE), lambda j: (layer, 0, here(j)))
    return pl.pallas_call(
        functools.partial(
            lift_kernel, row_count=row_count, blocks=blocks, mid=mid, layer=layer, parts=parts
        ),
        grid=(blocks + parts,),
        in_specs=[
            pl.BlockSpec((cells, 2, 8, WIDE), lambda j: (0, 0, 0, here(j))),
            pl.BlockSpec((members, 2, WIDE), lambda j: (0, 0, here(j))),
            pair, pair, pair, pair,
            pl.BlockSpec((1, mid, squeeze), lambda j: (layer, 0, 0)),
            pl.BlockSpec((LAYERS, squeeze), lambda j: (0, 0)),
            pl.BlockSpec((1, squeeze, mid), lambda j: (layer, 0, 0)),
            pl.BlockSpec((LAYERS, mid), lambda j: (0, 0)),
            pl.BlockSpec((1, mid, out), lambda j: (layer, 0, 0)),
            pl.BlockSpec((LAYERS, out), lambda j: (0, 0)),
        ],
        out_specs=[
            pl.BlockSpec((rows // parts, out), lambda j: (jnp.maximum(j - blocks, 0), 0)),
            pl.BlockSpec((members, 2, out), lambda j: (0, 0, 0)),
            pl.BlockSpec((2, WIDE), lambda j: (0, here(j))),
        ],
        out_shape=[
            jax.ShapeDtypeStruct((rows, out), jnp.float32),
            jax.ShapeDtypeStruct((members, 2, out), jnp.float32),
            jax.ShapeDtypeStruct((2, mid), jnp.float32),
        ],
        scratch_shapes=[
            pltpu.VMEM((blocks, cells, 2, 8, WIDE), jnp.float32),
            pltpu.VMEM((blocks, 16, WIDE), jnp.float32),
            pltpu.VMEM((blocks, 2, 8, WIDE), jnp.float32),
            pltpu.VMEM((rows // parts, mid), jnp.bfloat16),
            pltpu.VMEM((2, 8, out), jnp.float32),
        ],
        name="lift_project",
    )(
        spread, received, mid_mean, mid_var, mid_gain, mid_bias,
        squeeze_weight, squeeze_bias, excite_weight, excite_bias, project_weight, out_mean,
    )


def output_kernel(
    x_ref, proj_ref, recv_ref, mean_ref, var_ref, gain_ref, bias_ref, *rest, row_count, layer, chunk, follow
):
    if follow:
        w_ref, mid_mean_ref, next_ref, new_ref, stat_ref = rest
    else:
        next_ref, new_ref = rest

    def produce():
        at = slice(layer, layer + 1)
        scale, shift, new_mean, new_var = coefficients(
            recv_ref[...], row_count, mean_ref[at], var_ref[at], gain_ref[at], bias_ref[at]
        )
        new_ref[...] = jnp.concatenate([new_mean, new_var], axis=0)

        def step(i, carry):
            here = pl.ds(pl.multiple_of(i * 64, 64), 64)
            total = x_ref[here, :].astype(jnp.float32) + proj_ref[here, :] * scale + shift
            next_ref[here, :] = total.astype(jnp.bfloat16)
            return carry

        lax.fori_loop(0, x_ref.shape[0] // 64, step, 0)

    if follow:
        pl.when(pl.program_id(0) == 0)(produce)
        expand_moments(next_ref, w_ref, mid_mean_ref[0, 0:1], stat_ref, chunk)
    else:
        produce()


def output_call(x, projected, received, out_mean, out_var, out_gain, out_bias, layer, row_count, follow=None):
    rows, out = x.shape
    members = received.shape[0]
    whole = pl.BlockSpec((LAYERS, out), lambda j: (0, 0))
    flat = pl.BlockSpec((rows, out), lambda j: (0, 0))
    in_specs = [flat, flat, pl.BlockSpec((members, 2, out), lambda j: (0, 0, 0)), whole, whole, whole, whole]
    out_specs = [flat, pl.BlockSpec((2, out), lambda j: (0, 0))]
    out_shape = [jax.ShapeDtypeStruct((rows, out), jnp.bfloat16), jax.ShapeDtypeStruct((2, out), jnp.float32)]
    operands = [x, projected, received, out_mean, out_var, out_gain, out_bias]
    steps = 1
    if follow is not None:
        expand_weight, mid_mean, sharers = follow
        mid = expand_weight.shape[2]
        steps = pl.cdiv(mid, WIDE)
        in_specs += [
            pl.BlockSpec((1, out, WIDE), lambda j: (layer + 1, 0, j)),
            pl.BlockSpec((1, 2, WIDE), lambda j: (layer + 1, 0, j)),
        ]
        out_specs.append(pl.BlockSpec((sharers, 2, WIDE), lambda j: (0, 0, j)))
        out_shape.append(jax.ShapeDtypeStruct((sharers, 2, mid), jnp.float32))
        operands += [expand_weight, mid_mean]
    return pl.pallas_call(
        functools.partial(
            output_kernel, row_count=row_count, layer=layer, chunk=rows // 6, follow=follow is not None
        ),
        grid=(steps,),
        in_specs=in_specs,
        out_specs=out_specs,
        out_shape=out_shape,
        name="block_output",
    )(*operands)


def exchange(stats):
    sums = lax.all_to_all(stats, "row", split_axis=0, concat_axis=0, tiled=True)
    total = jnp.sum(sums, axis=0)
    copies = jnp.broadcast_to(total[None], (lax.axis_size("col"),) + total.shape)
    return lax.all_to_all(copies, "col", split_axis=0, concat_axis=0, tiled=True)


def per_device(
    images, expand_weight, depth_kernel, squeeze_weight, squeeze_bias, excite_weight, excite_bias,
    project_weight, mid_gain, mid_bias, out_gain, out_bias, mid_mean, mid_var, out_mean, out_var,
):
    batch, side, _, out = images.shape
    members = lax.axis_size("row")
    row_count = float(batch * side * side * members * lax.axis_size("col"))
    current = jnp.transpose(images, (1, 2, 0, 3)).reshape(side * side * batch, out)
    mid_new, out_new = [], []
    stats = moments_call(current, expand_weight, mid_mean, 0, members)
    for layer in range(LAYERS):
        received = exchange(stats)
        spread, stats, first_new = depth_call(
            current, expand_weight, depth_kernel, received, mid_mean, mid_var, mid_gain, mid_bias,
            layer, side, row_count,
        )
        received = exchange(stats)
        projected, stats, second_new = lift_call(
            spread, received, mid_mean, mid_var, mid_gain, mid_bias, squeeze_weight, squeeze_bias,
            excite_weight, excite_bias, project_weight, out_mean, layer, row_count,
        )
        received = exchange(stats)
        follow = (expand_weight, mid_mean, members) if layer + 1 < LAYERS else None
        results = output_call(
            current, projected, received, out_mean, out_var, out_gain, out_bias, layer, row_count, follow
        )
        current, third_new = results[0], results[1]
        if follow is not None:
            stats = results[2]
        mid_new.append(jnp.stack([first_new, second_new]))
        out_new.append(third_new)
    mid_new = jnp.stack(mid_new)
    out_new = jnp.stack(out_new)
    block_output = jnp.transpose(current.reshape(side, side, batch, out), (2, 0, 1, 3))
    return block_output, mid_new[:, :, 0], mid_new[:, :, 1], out_new[:, 0], out_new[:, 1]


def solution(mesh):
    split = P(("row", "col"), None, None, None)
    return jax.shard_map(
        per_device, mesh=mesh, in_specs=(split,) + (P(),) * 15, out_specs=(split, P(), P(), P(), P()), check_vma=False
    )
```

```python
import functools
import jax
import jax.numpy as jnp
from jax import lax
from jax.experimental import pallas as pl
from jax.experimental.pallas import tpu as pltpu
from jax.sharding import PartitionSpec as P

KERN = 5
LAYERS = 2
EPSILON = 0.001
RATIO_MAX = 3.0
SHIFT_MAX = 5.0
MOMENTUM = 0.01
LANE = 128
WIDE = 256


def coefficients(received, row_count, run_mean, run_var, gain, bias):
    sums = jnp.sum(received, axis=0)
    offset = sums[0:1] / row_count
    batch_var = sums[1:2] / row_count - offset * offset
    batch_mean = run_mean + offset
    batch_sigma = jnp.sqrt(batch_var + EPSILON)
    run_sigma = jnp.sqrt(run_var + EPSILON)
    scale_ratio = jnp.clip(batch_sigma / run_sigma, 1.0 / RATIO_MAX, RATIO_MAX)
    shift_clip = jnp.clip(offset / run_sigma, -SHIFT_MAX, SHIFT_MAX)
    gain_scale = gain * scale_ratio / batch_sigma
    gain_shift = bias + gain * shift_clip - batch_mean * gain_scale
    new_mean = run_mean + MOMENTUM * offset
    new_var = run_var + MOMENTUM * (batch_var - run_var)
    return gain_scale, gain_shift, new_mean, new_var


def half_silu(half):
    return half + half * jnp.tanh(half)


def fold_rows(block):
    return jnp.sum(block.reshape(block.shape[0] // 8, 8, block.shape[1]), axis=0)


def store_stats(stat_ref, first, second):
    members = stat_ref.shape[0]
    pair = jnp.concatenate(
        [jnp.sum(first, axis=0, keepdims=True), jnp.sum(second, axis=0, keepdims=True)], axis=0
    )
    stat_ref[...] = jnp.broadcast_to(pair[None], (members,) + pair.shape)


def expand_moments(x_ref, w_ref, mean, stat_ref, parts):
    chunk = x_ref.shape[0] // parts
    first = second = None
    for part in range(parts):
        values = jnp.dot(
            x_ref[part * chunk : (part + 1) * chunk, :], w_ref[0], preferred_element_type=jnp.float32
        )
        centered = values - mean
        one, two = fold_rows(centered), fold_rows(centered * centered)
        first = one if first is None else first + one
        second = two if second is None else second + two
    store_stats(stat_ref, first, second)


def moments_kernel(x_ref, w_ref, mean_ref, stat_ref, *, parts):
    expand_moments(x_ref, w_ref, mean_ref[0, 0:1], stat_ref, parts)


def moments_call(x, expand_weight, mid_mean, layer, members):
    rows, out = x.shape
    mid = expand_weight.shape[2]
    steps = pl.cdiv(mid, WIDE)
    return pl.pallas_call(
        functools.partial(moments_kernel, parts=3),
        grid=(steps,),
        in_specs=[
            pl.BlockSpec((rows, out), lambda j: (0, 0)),
            pl.BlockSpec((1, out, WIDE), lambda j: (layer, 0, j)),
            pl.BlockSpec((1, 2, WIDE), lambda j: (layer, 0, j)),
        ],
        out_specs=pl.BlockSpec((members, 2, WIDE), lambda j: (0, 0, j)),
        out_shape=jax.ShapeDtypeStruct((members, 2, mid), jnp.float32),
        name="expand_moments",
    )(x, expand_weight, mid_mean)


def depth_kernel_body(
    x_ref, w_ref, dk_ref, recv_ref, mean_ref, var_ref, gain_ref, bias_ref,
    spread_ref, stat_ref, new_ref, act_ref, tap_ref, *, row_count, side, parts, tail,
):
    j = pl.program_id(0)
    rows = x_ref.shape[0]
    reach = KERN // 2
    scale, shift, new_mean, new_var = coefficients(
        recv_ref[...], row_count, mean_ref[0, 0:1], var_ref[0, 0:1], gain_ref[0, 0:1], bias_ref[0, 0:1]
    )
    new_ref[...] = jnp.concatenate([new_mean, new_var], axis=0)
    scale = 0.5 * scale
    shift = 0.5 * shift
    chunk = rows // parts
    cells = chunk // 16
    for part in range(parts):
        values = jnp.dot(
            x_ref[part * chunk : (part + 1) * chunk, :], w_ref[0], preferred_element_type=jnp.float32
        )
        active = half_silu(values * scale + shift).astype(jnp.bfloat16).reshape(cells, 16, WIDE)
        for s in range(2):
            act_ref[s, part * cells : (part + 1) * cells] = active[:, :, s * LANE : (s + 1) * LANE]

    def lanes(s):
        here = slice(s * LANE, (s + 1) * LANE)
        mean = mean_ref[0, 1:2, here]
        for t in range(KERN * KERN):
            tap_ref[s, t] = jnp.broadcast_to(dk_ref[0, t : t + 1, here], (16, LANE)).astype(jnp.bfloat16)
        first = jnp.zeros((16, LANE), jnp.float32)
        second = jnp.zeros((16, LANE), jnp.float32)
        for h in range(side):
            for w in range(side):
                acc = None
                for i in range(KERN):
                    for k in range(KERN):
                        r, p = h + i - reach, w + k - reach
                        if 0 <= r < side and 0 <= p < side:
                            cell = act_ref[s, r * side + p].astype(jnp.float32)
                            term = cell * tap_ref[s, i * KERN + k].astype(jnp.float32)
                            acc = term if acc is None else acc + term
                spread_ref[h * side + w, :, here] = acc
                centered = acc - mean
                first = first + centered
                second = second + centered * centered
        pair = jnp.concatenate(
            [jnp.sum(first, axis=0, keepdims=True), jnp.sum(second, axis=0, keepdims=True)], axis=0
        )
        stat_ref[:, :, here] = jnp.broadcast_to(pair[None], (stat_ref.shape[0],) + pair.shape)

    lanes(0)
    if tail > LANE:
        lanes(1)
    else:
        pl.when(j < pl.num_programs(0) - 1)(lambda: lanes(1))


def depth_call(x, expand_weight, depth_kernel, received, mid_mean, mid_var, mid_gain, mid_bias, layer, side, row_count):
    rows, out = x.shape
    mid = expand_weight.shape[2]
    members = received.shape[0]
    cells = side * side
    steps = pl.cdiv(mid, WIDE)
    pair = pl.BlockSpec((1, 2, WIDE), lambda j: (layer, 0, j))
    return pl.pallas_call(
        functools.partial(
            depth_kernel_body, row_count=row_count, side=side, parts=3, tail=mid - (steps - 1) * WIDE
        ),
        grid=(steps,),
        in_specs=[
            pl.BlockSpec((rows, out), lambda j: (0, 0)),
            pl.BlockSpec((1, out, WIDE), lambda j: (layer, 0, j)),
            pl.BlockSpec((1, KERN * KERN, WIDE), lambda j: (layer, 0, j)),
            pl.BlockSpec((members, 2, WIDE), lambda j: (0, 0, j)),
            pair, pair, pair, pair,
        ],
        out_specs=[
            pl.BlockSpec((cells, 16, WIDE), lambda j: (0, 0, j)),
            pl.BlockSpec((members, 2, WIDE), lambda j: (0, 0, j)),
            pl.BlockSpec((2, WIDE), lambda j: (0, j)),
        ],
        out_shape=[
            jax.ShapeDtypeStruct((cells, 16, mid), jnp.float32),
            jax.ShapeDtypeStruct((members, 2, mid), jnp.float32),
            jax.ShapeDtypeStruct((2, mid), jnp.float32),
        ],
        scratch_shapes=[
            pltpu.VMEM((2, cells, 16, LANE), jnp.bfloat16),
            pltpu.VMEM((2, KERN * KERN, 16, LANE), jnp.bfloat16),
        ],
        name="depthwise",
    )(x, expand_weight, depth_kernel, received, mid_mean, mid_var, mid_gain, mid_bias)


def lift_kernel(
    spread_ref, recv_ref, mean_ref, var_ref, gain_ref, bias_ref,
    w1_ref, b1_ref, w2_ref, b2_ref, wp_ref, mean3_ref,
    proj_ref, stat_ref, new_ref,
    lift_ref, pool_ref, gate_ref, scaled_ref, sum_ref, *, row_count, blocks, mid, layer, parts,
):
    j = pl.program_id(0)
    cells = lift_ref.shape[1]
    group = cells // parts

    @pl.when(j < blocks)
    def _():
        scale, shift, new_mean, new_var = coefficients(
            recv_ref[...], row_count, mean_ref[0, 1:2], var_ref[0, 1:2], gain_ref[0, 1:2], bias_ref[0, 1:2]
        )
        new_ref[...] = jnp.concatenate([new_mean, new_var], axis=0)
        scale = 0.5 * scale
        shift = 0.5 * shift

        def step(i, pooled):
            at = pl.multiple_of(i * 16, 16)
            values = spread_ref[pl.ds(at, 16)]
            lifted = half_silu(values * scale + shift)
            lift_ref[j, pl.ds(at, 16)] = lifted
            return pooled + jnp.sum(lifted, axis=0)

        pooled = lax.fori_loop(0, cells // 16, step, jnp.zeros((16, WIDE), jnp.float32))
        pool_ref[j] = pooled * (1.0 / cells)

    @pl.when(j == blocks)
    def _():
        last = mid - (blocks - 1) * WIDE
        squeezed = b1_ref[layer : layer + 1, :] + jnp.zeros((16, b1_ref.shape[1]), jnp.float32)
        for k in range(blocks):
            size = WIDE if k < blocks - 1 else last
            squeezed = squeezed + jnp.dot(
                pool_ref[k, :, :size], w1_ref[0, k * WIDE : k * WIDE + size, :],
                precision=lax.Precision.HIGHEST, preferred_element_type=jnp.float32,
            )
        squeezed = half_silu(0.5 * squeezed)
        for k in range(blocks):
            size = WIDE if k < blocks - 1 else last
            grown = jnp.dot(
                squeezed, w2_ref[0, :, k * WIDE : k * WIDE + size],
                precision=lax.Precision.HIGHEST, preferred_element_type=jnp.float32,
            ) + b2_ref[layer : layer + 1, k * WIDE : k * WIDE + size]
            gate_ref[k, :, :size] = jax.nn.sigmoid(grown)

    @pl.when(j >= blocks)
    def _():
        part = j - blocks
        base = pl.multiple_of(part * group, group)
        last = mid - (blocks - 1) * WIDE
        for k in range(blocks):
            size = WIDE if k < blocks - 1 else last
            gate = gate_ref[k, :, :size]
            lifted = lift_ref[k, pl.ds(base, group), :, :size]
            scaled = (lifted * gate).reshape(group * 16, size).astype(jnp.bfloat16)
            scaled_ref[:, k * WIDE : k * WIDE + size] = scaled
        projected = jnp.dot(scaled_ref[...], wp_ref[0], preferred_element_type=jnp.float32)
        proj_ref[...] = projected
        centered = projected - mean3_ref[layer : layer + 1, :]
        first = fold_rows(centered)
        second = fold_rows(centered * centered)

        @pl.when(part == 0)
        def _():
            sum_ref[0] = first
            sum_ref[1] = second

        @pl.when(part > 0)
        def _():
            sum_ref[0] += first
            sum_ref[1] += second

        @pl.when(part == parts - 1)
        def _():
            store_stats(stat_ref, sum_ref[0], sum_ref[1])


def lift_call(
    spread, received, mid_mean, mid_var, mid_gain, mid_bias,
    squeeze_weight, squeeze_bias, excite_weight, excite_bias, project_weight, out_mean, layer, row_count,
):
    cells, _, mid = spread.shape
    members = received.shape[0]
    out = project_weight.shape[2]
    squeeze = squeeze_weight.shape[2]
    blocks = pl.cdiv(mid, WIDE)
    parts = 3
    rows = cells * 16
    here = lambda j: jnp.minimum(j, blocks - 1)
    pair = pl.BlockSpec((1, 2, WIDE), lambda j: (layer, 0, here(j)))
    return pl.pallas_call(
        functools.partial(
            lift_kernel, row_count=row_count, blocks=blocks, mid=mid, layer=layer, parts=parts
        ),
        grid=(blocks + parts,),
        in_specs=[
            pl.BlockSpec((cells, 16, WIDE), lambda j: (0, 0, here(j))),
            pl.BlockSpec((members, 2, WIDE), lambda j: (0, 0, here(j))),
            pair, pair, pair, pair,
            pl.BlockSpec((1, mid, squeeze), lambda j: (layer, 0, 0)),
            pl.BlockSpec((LAYERS, squeeze), lambda j: (0, 0)),
            pl.BlockSpec((1, squeeze, mid), lambda j: (layer, 0, 0)),
            pl.BlockSpec((LAYERS, mid), lambda j: (0, 0)),
            pl.BlockSpec((1, mid, out), lambda j: (layer, 0, 0)),
            pl.BlockSpec((LAYERS, out), lambda j: (0, 0)),
        ],
        out_specs=[
            pl.BlockSpec((rows // parts, out), lambda j: (jnp.maximum(j - blocks, 0), 0)),
            pl.BlockSpec((members, 2, out), lambda j: (0, 0, 0)),
            pl.BlockSpec((2, WIDE), lambda j: (0, here(j))),
        ],
        out_shape=[
            jax.ShapeDtypeStruct((rows, out), jnp.float32),
            jax.ShapeDtypeStruct((members, 2, out), jnp.float32),
            jax.ShapeDtypeStruct((2, mid), jnp.float32),
        ],
        scratch_shapes=[
            pltpu.VMEM((blocks, cells, 16, WIDE), jnp.float32),
            pltpu.VMEM((blocks, 16, WIDE), jnp.float32),
            pltpu.VMEM((blocks, 16, WIDE), jnp.float32),
            pltpu.VMEM((rows // parts, mid), jnp.bfloat16),
            pltpu.VMEM((2, 8, out), jnp.float32),
        ],
        name="lift_project",
    )(
        spread, received, mid_mean, mid_var, mid_gain, mid_bias,
        squeeze_weight, squeeze_bias, excite_weight, excite_bias, project_weight, out_mean,
    )


def output_kernel(
    x_ref, proj_ref, recv_ref, mean_ref, var_ref, gain_ref, bias_ref, *rest, row_count, layer, parts, follow
):
    if follow:
        w_ref, mid_mean_ref, next_ref, new_ref, stat_ref = rest
    else:
        next_ref, new_ref = rest

    def produce():
        at = slice(layer, layer + 1)
        scale, shift, new_mean, new_var = coefficients(
            recv_ref[...], row_count, mean_ref[at], var_ref[at], gain_ref[at], bias_ref[at]
        )
        new_ref[...] = jnp.concatenate([new_mean, new_var], axis=0)

        def step(i, carry):
            here = pl.ds(pl.multiple_of(i * 128, 128), 128)
            total = x_ref[here, :].astype(jnp.float32) + proj_ref[here, :] * scale + shift
            next_ref[here, :] = total.astype(jnp.bfloat16)
            return carry

        lax.fori_loop(0, x_ref.shape[0] // 128, step, 0)

    if follow:
        pl.when(pl.program_id(0) == 0)(produce)
        expand_moments(next_ref, w_ref, mid_mean_ref[0, 0:1], stat_ref, parts)
    else:
        produce()


def output_call(x, projected, received, out_mean, out_var, out_gain, out_bias, layer, row_count, follow=None):
    rows, out = x.shape
    members = received.shape[0]
    whole = pl.BlockSpec((LAYERS, out), lambda j: (0, 0))
    flat = pl.BlockSpec((rows, out), lambda j: (0, 0))
    in_specs = [flat, flat, pl.BlockSpec((members, 2, out), lambda j: (0, 0, 0)), whole, whole, whole, whole]
    out_specs = [flat, pl.BlockSpec((2, out), lambda j: (0, 0))]
    out_shape = [jax.ShapeDtypeStruct((rows, out), jnp.bfloat16), jax.ShapeDtypeStruct((2, out), jnp.float32)]
    operands = [x, projected, received, out_mean, out_var, out_gain, out_bias]
    steps = 1
    if follow is not None:
        expand_weight, mid_mean, sharers = follow
        mid = expand_weight.shape[2]
        steps = pl.cdiv(mid, WIDE)
        in_specs += [
            pl.BlockSpec((1, out, WIDE), lambda j: (layer + 1, 0, j)),
            pl.BlockSpec((1, 2, WIDE), lambda j: (layer + 1, 0, j)),
        ]
        out_specs.append(pl.BlockSpec((sharers, 2, WIDE), lambda j: (0, 0, j)))
        out_shape.append(jax.ShapeDtypeStruct((sharers, 2, mid), jnp.float32))
        operands += [expand_weight, mid_mean]
    return pl.pallas_call(
        functools.partial(
            output_kernel, row_count=row_count, layer=layer, parts=3, follow=follow is not None
        ),
        grid=(steps,),
        in_specs=in_specs,
        out_specs=out_specs,
        out_shape=out_shape,
        name="block_output",
    )(*operands)


def exchange(stats):
    sums = lax.all_to_all(stats, "row", split_axis=0, concat_axis=0, tiled=True)
    total = jnp.sum(sums, axis=0)
    copies = jnp.broadcast_to(total[None], (lax.axis_size("col"),) + total.shape)
    return lax.all_to_all(copies, "col", split_axis=0, concat_axis=0, tiled=True)


def per_device(
    images, expand_weight, depth_kernel, squeeze_weight, squeeze_bias, excite_weight, excite_bias,
    project_weight, mid_gain, mid_bias, out_gain, out_bias, mid_mean, mid_var, out_mean, out_var,
):
    batch, side, _, out = images.shape
    members = lax.axis_size("row")
    row_count = float(batch * side * side * members * lax.axis_size("col"))
    current = jnp.transpose(images, (1, 2, 0, 3)).reshape(side * side * batch, out)
    mid_new, out_new = [], []
    stats = moments_call(current, expand_weight, mid_mean, 0, members)
    for layer in range(LAYERS):
        received = exchange(stats)
        spread, stats, first_new = depth_call(
            current, expand_weight, depth_kernel, received, mid_mean, mid_var, mid_gain, mid_bias,
            layer, side, row_count,
        )
        received = exchange(stats)
        projected, stats, second_new = lift_call(
            spread, received, mid_mean, mid_var, mid_gain, mid_bias, squeeze_weight, squeeze_bias,
            excite_weight, excite_bias, project_weight, out_mean, layer, row_count,
        )
        received = exchange(stats)
        follow = (expand_weight, mid_mean, members) if layer + 1 < LAYERS else None
        results = output_call(
            current, projected, received, out_mean, out_var, out_gain, out_bias, layer, row_count, follow
        )
        current, third_new = results[0], results[1]
        if follow is not None:
            stats = results[2]
        mid_new.append(jnp.stack([first_new, second_new]))
        out_new.append(third_new)
    mid_new = jnp.stack(mid_new)
    out_new = jnp.stack(out_new)
    block_output = jnp.transpose(current.reshape(side, side, batch, out), (2, 0, 1, 3))
    return block_output, mid_new[:, :, 0], mid_new[:, :, 1], out_new[:, 0], out_new[:, 1]


def solution(mesh):
    split = P(("row", "col"), None, None, None)
    return jax.shard_map(
        per_device, mesh=mesh, in_specs=(split,) + (P(),) * 15, out_specs=(split, P(), P(), P(), P()), check_vma=False
    )
```

```python
import functools
import jax
import jax.numpy as jnp
from jax import lax
from jax.experimental import pallas as pl
from jax.experimental.pallas import tpu as pltpu
from jax.sharding import PartitionSpec as P

KERN = 5
LAYERS = 2
EPSILON = 0.001
RATIO_MAX = 3.0
SHIFT_MAX = 5.0
MOMENTUM = 0.01
LANE = 128
WIDE = 256
MIB = 1 << 20


def coefficients(sums, row_count, run_mean, run_var, gain, bias):
    offset = sums[0] / row_count
    batch_var = sums[1] / row_count - offset * offset
    batch_mean = run_mean + offset
    batch_sigma = jnp.sqrt(batch_var + EPSILON)
    run_sigma = jnp.sqrt(run_var + EPSILON)
    scale_ratio = jnp.clip(batch_sigma / run_sigma, 1.0 / RATIO_MAX, RATIO_MAX)
    shift_clip = jnp.clip(offset / run_sigma, -SHIFT_MAX, SHIFT_MAX)
    gain_scale = gain * scale_ratio / batch_sigma
    gain_shift = bias + gain * shift_clip - batch_mean * gain_scale
    new_mean = run_mean + MOMENTUM * offset
    new_var = run_var + MOMENTUM * (batch_var - run_var)
    return jnp.stack([gain_scale, gain_shift]), new_mean, new_var


def half_silu(half):
    return half + half * jnp.tanh(half)


def fold_rows(block):
    return jnp.sum(block.reshape(block.shape[0] // 8, 8, block.shape[1]), axis=0)


def stat_copies(first, second, members):
    pair = jnp.concatenate(
        [jnp.sum(first, axis=0, keepdims=True), jnp.sum(second, axis=0, keepdims=True)], axis=0
    )
    return jnp.broadcast_to(pair[None], (members,) + pair.shape)


def call(kernel, name, out_shape, scratch, limit, *operands):
    return pl.pallas_call(
        kernel,
        in_specs=[pl.BlockSpec(memory_space=pltpu.VMEM)] * len(operands),
        out_specs=[pl.BlockSpec(memory_space=pltpu.VMEM)] * len(out_shape),
        out_shape=out_shape,
        scratch_shapes=scratch,
        compiler_params=pltpu.CompilerParams(vmem_limit_bytes=limit * MIB),
        name=name,
    )(*operands)


def expand_moments(x_ref, w_ref, mean_ref, stat_ref, layer, parts):
    rows = x_ref.shape[0]
    mid = w_ref.shape[2]
    chunk = rows // parts

    def lanes(here):
        mean = mean_ref[layer, 0:1, here]
        first = second = None
        for part in range(parts):
            values = jnp.dot(
                x_ref[part * chunk : (part + 1) * chunk, :], w_ref[layer, :, here],
                preferred_element_type=jnp.float32,
            )
            centered = values - mean
            one, two = fold_rows(centered), fold_rows(centered * centered)
            first = one if first is None else first + one
            second = two if second is None else second + two
        stat_ref[:, :, here] = stat_copies(first, second, stat_ref.shape[0])

    def step(j, carry):
        lanes(pl.ds(pl.multiple_of(j * WIDE, WIDE), WIDE))
        return carry

    full = mid // WIDE
    lax.fori_loop(0, full, step, 0)
    if mid > full * WIDE:
        lanes(slice(full * WIDE, mid))


def moments_kernel(x_ref, w_ref, mean_ref, stat_ref, *, layer, parts):
    expand_moments(x_ref, w_ref, mean_ref, stat_ref, layer, parts)


def moments_call(x, expand_weight, mid_mean, layer, members):
    mid = expand_weight.shape[2]
    return call(
        functools.partial(moments_kernel, layer=layer, parts=3),
        "expand_moments",
        [jax.ShapeDtypeStruct((members, 2, mid), jnp.float32)],
        [], 24, x, expand_weight, mid_mean,
    )[0]


def depth_kernel_body(
    x_ref, w_ref, dk_ref, coef_ref, mean_ref, spread_ref, stat_ref, act_ref, tap_ref, *, layer, side, parts
):
    rows = x_ref.shape[0]
    mid = stat_ref.shape[2]
    blocks = spread_ref.shape[0]
    reach = KERN // 2
    chunk = rows // parts
    cells = chunk // 16

    def activate(start, width):
        here = pl.ds(start, width)
        scale = 0.5 * coef_ref[0:1, here]
        shift = 0.5 * coef_ref[1:2, here]
        for part in range(parts):
            values = jnp.dot(
                x_ref[part * chunk : (part + 1) * chunk, :], w_ref[layer, :, here],
                preferred_element_type=jnp.float32,
            )
            active = half_silu(values * scale + shift).astype(jnp.bfloat16).reshape(cells, 16, width)
            for s in range(width // LANE):
                act_ref[s, part * cells : (part + 1) * cells] = active[:, :, s * LANE : (s + 1) * LANE]

    def spread_block(s, block, start, size):
        here = pl.ds(start, LANE)
        mean = mean_ref[layer, 1:2, here]
        for t in range(KERN * KERN):
            tap_ref[s, t] = jnp.broadcast_to(dk_ref[layer, t : t + 1, here], (16, LANE)).astype(jnp.bfloat16)
        first = jnp.zeros((16, LANE), jnp.float32)
        second = jnp.zeros((16, LANE), jnp.float32)
        for h in range(side):
            for w in range(side):
                acc = None
                for i in range(KERN):
                    for k in range(KERN):
                        r, p = h + i - reach, w + k - reach
                        if 0 <= r < side and 0 <= p < side:
                            cell = act_ref[s, r * side + p].astype(jnp.float32)
                            term = cell * tap_ref[s, i * KERN + k].astype(jnp.float32)
                            acc = term if acc is None else acc + term
                spread_ref[block, h * side + w] = acc
                centered = acc - mean
                first = first + centered
                second = second + centered * centered
        copies = stat_copies(first, second, stat_ref.shape[0])
        stat_ref[:, :, pl.ds(start, size)] = copies[:, :, :size]

    def step(j, carry):
        start = pl.multiple_of(j * WIDE, WIDE)
        activate(start, WIDE)
        spread_block(0, 2 * j, start, LANE)
        spread_block(1, 2 * j + 1, pl.multiple_of(start + LANE, LANE), LANE)
        return carry

    lax.fori_loop(0, blocks // 2, step, 0)
    if blocks % 2:
        start = (blocks - 1) * LANE
        activate(start, LANE)
        spread_block(0, blocks - 1, start, mid - start)


def depth_call(x, expand_padded, kernel_padded, coef, mean_padded, mid, members, layer, side):
    blocks = expand_padded.shape[2] // LANE
    cells = side * side
    return call(
        functools.partial(depth_kernel_body, layer=layer, side=side, parts=3),
        "depthwise",
        [
            jax.ShapeDtypeStruct((blocks, cells, 16, LANE), jnp.float32),
            jax.ShapeDtypeStruct((members, 2, mid), jnp.float32),
        ],
        [
            pltpu.VMEM((2, cells, 16, LANE), jnp.bfloat16),
            pltpu.VMEM((2, KERN * KERN, 16, LANE), jnp.bfloat16),
        ],
        28, x, expand_padded, kernel_padded, coef, mean_padded,
    )


def lift_kernel(
    spread_ref, coef_ref, w1_ref, b1_ref, w2_ref, b2_ref, wp_ref, mean3_ref, proj_ref, stat_ref,
    lift_ref, pool_ref, gate_ref, scaled_ref, *, layer, parts,
):
    blocks, cells = spread_ref.shape[0], spread_ref.shape[1]
    mid = w1_ref.shape[1]
    at = slice(layer, layer + 1)
    batch = 24

    def block_step(j, carry):
        here = pl.ds(pl.multiple_of(j * LANE, LANE), LANE)
        scale = 0.5 * coef_ref[0:1, here]
        shift = 0.5 * coef_ref[1:2, here]

        def step(i, pooled):
            cell = pl.multiple_of(i * batch, batch)
            lifted = half_silu(spread_ref[j, pl.ds(cell, batch)] * scale + shift)
            lift_ref[j, pl.ds(cell, batch)] = lifted
            return pooled + jnp.sum(lifted, axis=0)

        pooled = lax.fori_loop(0, cells // batch, step, jnp.zeros((16, LANE), jnp.float32))
        pool_ref[:, here] = pooled * (1.0 / cells)
        return carry

    lax.fori_loop(0, blocks, block_step, 0)

    squeezed = b1_ref[at, :] + jnp.dot(
        pool_ref[:, :mid], w1_ref[layer], precision=lax.Precision.HIGHEST, preferred_element_type=jnp.float32
    )
    squeezed = half_silu(0.5 * squeezed)
    grown = b2_ref[at, :] + jnp.dot(
        squeezed, w2_ref[layer], precision=lax.Precision.HIGHEST, preferred_element_type=jnp.float32
    )
    gate_ref[:, :mid] = 0.5 + 0.5 * jnp.tanh(0.5 * grown)

    group = cells // parts
    out = proj_ref.shape[1]

    def part_step(part, carry):
        first, second = carry
        base = pl.multiple_of(part * group, group)
        for k in range(blocks):
            size = min(LANE, mid - k * LANE)
            gate = gate_ref[:, k * LANE : k * LANE + size]
            scaled = (lift_ref[k, pl.ds(base, group), :, :size] * gate).reshape(group * 16, size)
            scaled_ref[:, k * LANE : k * LANE + size] = scaled.astype(jnp.bfloat16)
        projected = jnp.dot(scaled_ref[...], wp_ref[layer], preferred_element_type=jnp.float32)
        proj_ref[pl.ds(pl.multiple_of(part * group * 16, group * 16), group * 16), :] = projected
        centered = projected - mean3_ref[at, :]
        return first + fold_rows(centered), second + fold_rows(centered * centered)

    zero = jnp.zeros((8, out), jnp.float32)
    first, second = lax.fori_loop(0, parts, part_step, (zero, zero))
    stat_ref[...] = stat_copies(first, second, stat_ref.shape[0])


def lift_call(
    spread, coef, squeeze_weight, squeeze_bias, excite_weight, excite_bias, project_weight, out_mean, layer, members
):
    blocks, cells = spread.shape[:2]
    mid, out = project_weight.shape[1:]
    parts = 3
    rows = cells * 16
    return call(
        functools.partial(lift_kernel, layer=layer, parts=parts),
        "lift_project",
        [
            jax.ShapeDtypeStruct((rows, out), jnp.float32),
            jax.ShapeDtypeStruct((members, 2, out), jnp.float32),
        ],
        [
            pltpu.VMEM((blocks, cells, 16, LANE), jnp.float32),
            pltpu.VMEM((16, blocks * LANE), jnp.float32),
            pltpu.VMEM((16, blocks * LANE), jnp.float32),
            pltpu.VMEM((rows // parts, mid), jnp.bfloat16),
        ],
        44, spread, coef, squeeze_weight, squeeze_bias, excite_weight, excite_bias, project_weight, out_mean,
    )


def output_kernel(x_ref, proj_ref, coef_ref, *rest, layer, parts):
    if len(rest) > 1:
        w_ref, mid_mean_ref, next_ref, stat_ref = rest
    else:
        (next_ref,) = rest
    scale = coef_ref[0:1, :]
    shift = coef_ref[1:2, :]

    def step(i, carry):
        here = pl.ds(pl.multiple_of(i * 192, 192), 192)
        total = x_ref[here, :].astype(jnp.float32) + proj_ref[here, :] * scale + shift
        next_ref[here, :] = total.astype(jnp.bfloat16)
        return carry

    lax.fori_loop(0, x_ref.shape[0] // 192, step, 0)
    if len(rest) > 1:
        expand_moments(next_ref, w_ref, mid_mean_ref, stat_ref, layer + 1, parts)


def output_call(x, projected, coef, layer, members, follow=None):
    rows, out = x.shape
    out_shape = [jax.ShapeDtypeStruct((rows, out), jnp.bfloat16)]
    operands = [x, projected, coef]
    if follow is not None:
        out_shape.append(jax.ShapeDtypeStruct((members, 2, follow[0].shape[2]), jnp.float32))
        operands += list(follow)
    return call(
        functools.partial(output_kernel, layer=layer, parts=3), "block_output", out_shape, [], 24, *operands
    )


def exchange(stats):
    sums = lax.all_to_all(stats, "row", split_axis=0, concat_axis=0, tiled=True)
    total = jnp.sum(sums, axis=0)
    copies = jnp.broadcast_to(total[None], (lax.axis_size("col"),) + total.shape)
    return jnp.sum(lax.all_to_all(copies, "col", split_axis=0, concat_axis=0, tiled=True), axis=0)


def per_device(
    images, expand_weight, depth_kernel, squeeze_weight, squeeze_bias, excite_weight, excite_bias,
    project_weight, mid_gain, mid_bias, out_gain, out_bias, mid_mean, mid_var, out_mean, out_var,
):
    batch, side, _, out = images.shape
    mid = expand_weight.shape[2]
    members = lax.axis_size("row")
    row_count = float(batch * side * side * members * lax.axis_size("col"))
    spare = -mid % LANE
    widen = lambda a: jnp.pad(a, [(0, 0)] * (a.ndim - 1) + [(0, spare)])
    current = jnp.transpose(images, (1, 2, 0, 3)).reshape(side * side * batch, out)
    mean_new, var_new, out_mean_new, out_var_new = [], [], [], []
    stats = moments_call(current, expand_weight, mid_mean, 0, members)
    expand_padded, kernel_padded, mean_padded = widen(expand_weight), widen(depth_kernel), widen(mid_mean)
    for layer in range(LAYERS):
        settle = lambda sums, k: coefficients(
            sums, row_count, mid_mean[layer, k], mid_var[layer, k], mid_gain[layer, k], mid_bias[layer, k]
        )
        coef, mean_a, var_a = settle(exchange(stats), 0)
        spread, stats = depth_call(
            current, expand_padded, kernel_padded, widen(coef), mean_padded, mid, members, layer, side
        )
        coef, mean_b, var_b = settle(exchange(stats), 1)
        projected, stats = lift_call(
            spread, widen(coef), squeeze_weight, squeeze_bias, excite_weight, excite_bias,
            project_weight, out_mean, layer, members,
        )
        coef, mean_c, var_c = coefficients(
            exchange(stats), row_count, out_mean[layer], out_var[layer], out_gain[layer], out_bias[layer]
        )
        if layer + 1 < LAYERS:
            current, stats = output_call(current, projected, coef, layer, members, (expand_weight, mid_mean))
        else:
            (current,) = output_call(current, projected, coef, layer, members)
        mean_new.append(jnp.stack([mean_a, mean_b]))
        var_new.append(jnp.stack([var_a, var_b]))
        out_mean_new.append(mean_c)
        out_var_new.append(var_c)
    block_output = jnp.transpose(current.reshape(side, side, batch, out), (2, 0, 1, 3))
    return (
        block_output, jnp.stack(mean_new), jnp.stack(var_new), jnp.stack(out_mean_new), jnp.stack(out_var_new)
    )


def solution(mesh):
    split = P(("row", "col"), None, None, None)
    return jax.shard_map(
        per_device, mesh=mesh, in_specs=(split,) + (P(),) * 15, out_specs=(split, P(), P(), P(), P()), check_vma=False
    )
```

```python
import functools
import jax
import jax.numpy as jnp
from jax import lax
from jax.experimental import pallas as pl
from jax.experimental.pallas import tpu as pltpu
from jax.sharding import PartitionSpec as P

KERN = 5
LAYERS = 2
EPSILON = 0.001
RATIO_MAX = 3.0
SHIFT_MAX = 5.0
MOMENTUM = 0.01
LANE = 128
WIDE = 256
MIB = 1 << 20


def coefficients(received, row_count, run_mean, run_var, gain, bias):
    offset = received[0:1] / row_count
    batch_var = received[1:2] / row_count - offset * offset
    batch_mean = run_mean + offset
    batch_sigma = jnp.sqrt(batch_var + EPSILON)
    run_sigma = jnp.sqrt(run_var + EPSILON)
    scale_ratio = jnp.clip(batch_sigma / run_sigma, 1.0 / RATIO_MAX, RATIO_MAX)
    shift_clip = jnp.clip(offset / run_sigma, -SHIFT_MAX, SHIFT_MAX)
    gain_scale = gain * scale_ratio / batch_sigma
    gain_shift = bias + gain * shift_clip - batch_mean * gain_scale
    new_mean = run_mean + MOMENTUM * offset
    new_var = run_var + MOMENTUM * (batch_var - run_var)
    return gain_scale, gain_shift, new_mean, new_var


def settle(recv_ref, param_ref, at, coef_ref, new_ref, row_count):
    size = recv_ref.shape[1]
    coef_ref[...] = jnp.zeros(coef_ref.shape, jnp.float32)
    coef_ref[:, :size] = recv_ref[...]
    index, half = at
    mean, var, gain, bias = [param_ref[4 * index + n : 4 * index + n + 1, :] for n in range(4)]
    scale, shift, new_mean, new_var = coefficients(coef_ref[...], row_count, mean, var, gain, bias)
    coef_ref[...] = half * jnp.concatenate([scale, shift], axis=0)
    new_ref[...] = jnp.concatenate([new_mean, new_var], axis=0)[:, :size]


def start_copies(pairs, sems):
    copies = [pltpu.make_async_copy(source, target, sems.at[n]) for n, (source, target) in enumerate(pairs)]
    for copy in copies:
        copy.start()
    return copies


def half_silu(half):
    return half + half * jnp.tanh(half)


def fold_rows(block):
    return jnp.sum(block.reshape(block.shape[0] // 8, 8, block.shape[1]), axis=0)


def stat_copies(first, second, members):
    pair = jnp.concatenate(
        [jnp.sum(first, axis=0, keepdims=True), jnp.sum(second, axis=0, keepdims=True)], axis=0
    )
    return jnp.broadcast_to(pair[None], (members,) + pair.shape)


def call(kernel, name, in_vmem, outs, scratch, limit, *operands):
    spec = lambda inside: pl.BlockSpec(memory_space=pltpu.VMEM if inside else pltpu.HBM)
    return pl.pallas_call(
        kernel,
        in_specs=[spec(n in in_vmem) for n in range(len(operands))],
        out_specs=[spec(inside) for _, inside in outs],
        out_shape=[shape for shape, _ in outs],
        scratch_shapes=scratch,
        compiler_params=pltpu.CompilerParams(vmem_limit_bytes=62 * MIB),
        name=name,
    )(*operands)


def expand_moments(x_ref, w_ref, mean_ref, stat_ref, parts):
    rows = x_ref.shape[0]
    mid = w_ref.shape[1]
    chunk = rows // parts

    def lanes(here):
        mean = mean_ref[0:1, here]
        first = second = None
        for part in range(parts):
            values = jnp.dot(
                x_ref[part * chunk : (part + 1) * chunk, :], w_ref[:, here],
                preferred_element_type=jnp.float32,
            )
            centered = values - mean
            one, two = fold_rows(centered), fold_rows(centered * centered)
            first = one if first is None else first + one
            second = two if second is None else second + two
        stat_ref[:, :, here] = stat_copies(first, second, stat_ref.shape[0])

    def step(j, carry):
        lanes(pl.ds(pl.multiple_of(j * WIDE, WIDE), WIDE))
        return carry

    full = mid // WIDE
    lax.fori_loop(0, full, step, 0)
    if mid > full * WIDE:
        lanes(slice(full * WIDE, mid))


def moments_kernel(x_hbm, w_hbm, mean_hbm, stat_ref, x_ref, w_ref, mean_ref, sems, *, layer, parts):
    pairs = [(x_hbm, x_ref), (w_hbm.at[layer], w_ref), (mean_hbm.at[layer], mean_ref)]
    for copy in start_copies(pairs, sems):
        copy.wait()
    expand_moments(x_ref, w_ref, mean_ref, stat_ref, parts)


def moments_call(x, expand_weight, mid_mean, layer, members):
    _, out, mid = expand_weight.shape
    return call(
        functools.partial(moments_kernel, layer=layer, parts=3),
        "expand_moments", (),
        [(jax.ShapeDtypeStruct((members, 2, mid), jnp.float32), True)],
        [
            pltpu.VMEM(x.shape, x.dtype),
            pltpu.VMEM((out, mid), expand_weight.dtype),
            pltpu.VMEM((2, mid), jnp.float32),
            pltpu.SemaphoreType.DMA((3,)),
        ],
        20, x, expand_weight, mid_mean,
    )[0]


def depth_kernel_body(
    x_hbm, w_hbm, dk_hbm, param_hbm, recv_hbm, spread_hbm, stat_ref, new_ref,
    recv_ref, spread_ref, x_ref, w_ref, dk_ref, param_ref, coef_ref, act_ref, tap_ref, in_sems, out_sems,
    *, layer, side, parts, row_count,
):
    copies = start_copies(
        [
            (recv_hbm, recv_ref), (param_hbm, param_ref), (x_hbm, x_ref), (w_hbm.at[layer], w_ref),
            (dk_hbm.at[layer], dk_ref),
        ],
        in_sems,
    )
    for copy in copies[:2]:
        copy.wait()
    settle(recv_ref, param_ref, (2 * layer, 0.5), coef_ref, new_ref, row_count)
    for copy in copies[2:]:
        copy.wait()
    rows = x_ref.shape[0]
    mid = stat_ref.shape[2]
    blocks = spread_ref.shape[0]
    reach = KERN // 2
    chunk = rows // parts
    cells = chunk // 16

    def leave(block):
        return pltpu.make_async_copy(spread_ref.at[block], spread_hbm.at[block], out_sems.at[block])

    def activate(start, width):
        here = pl.ds(start, width)
        scale = coef_ref[0:1, here]
        shift = coef_ref[1:2, here]
        for part in range(parts):
            values = jnp.dot(
                x_ref[part * chunk : (part + 1) * chunk, :], w_ref[:, here],
                preferred_element_type=jnp.float32,
            )
            active = half_silu(values * scale + shift).astype(jnp.bfloat16).reshape(cells, 16, width)
            for s in range(width // LANE):
                act_ref[s, part * cells : (part + 1) * cells] = active[:, :, s * LANE : (s + 1) * LANE]

    def spread_block(s, block, start, size):
        here = pl.ds(start, LANE)
        mean = param_ref[8 * layer + 4 : 8 * layer + 5, here]
        for t in range(KERN * KERN):
            tap_ref[s, t] = jnp.broadcast_to(dk_ref[t : t + 1, here], (16, LANE)).astype(jnp.bfloat16)
        first = jnp.zeros((16, LANE), jnp.float32)
        second = jnp.zeros((16, LANE), jnp.float32)
        for h in range(side):
            for w in range(side):
                acc = None
                for i in range(KERN):
                    for k in range(KERN):
                        r, p = h + i - reach, w + k - reach
                        if 0 <= r < side and 0 <= p < side:
                            cell = act_ref[s, r * side + p].astype(jnp.float32)
                            term = cell * tap_ref[s, i * KERN + k].astype(jnp.float32)
                            acc = term if acc is None else acc + term
                spread_ref[block, h * side + w] = acc
                centered = acc - mean
                first = first + centered
                second = second + centered * centered
        copies = stat_copies(first, second, stat_ref.shape[0])
        stat_ref[:, :, pl.ds(start, size)] = copies[:, :, :size]
        leave(block).start()

    def step(j, carry):
        start = pl.multiple_of(j * WIDE, WIDE)
        activate(start, WIDE)
        spread_block(0, 2 * j, start, LANE)
        spread_block(1, 2 * j + 1, pl.multiple_of(start + LANE, LANE), LANE)
        return carry

    lax.fori_loop(0, blocks // 2, step, 0)
    if blocks % 2:
        start = (blocks - 1) * LANE
        activate(start, LANE)
        spread_block(0, blocks - 1, start, mid - start)
    for block in range(blocks):
        leave(block).wait()


def depth_call(x, expand_padded, kernel_padded, params, received, members, layer, side, row_count):
    _, out, padded = expand_padded.shape
    mid = received.shape[1]
    blocks = padded // LANE
    field = (blocks, side * side, 16, LANE)
    return call(
        functools.partial(depth_kernel_body, layer=layer, side=side, parts=3, row_count=row_count),
        "depthwise", (),
        [
            (jax.ShapeDtypeStruct(field, jnp.float32), False),
            (jax.ShapeDtypeStruct((members, 2, mid), jnp.float32), True),
            (jax.ShapeDtypeStruct((2, mid), jnp.float32), True),
        ],
        [
            pltpu.VMEM(received.shape, jnp.float32),
            pltpu.VMEM(field, jnp.float32),
            pltpu.VMEM(x.shape, x.dtype),
            pltpu.VMEM((out, padded), expand_padded.dtype),
            pltpu.VMEM(kernel_padded.shape[1:], jnp.float32),
            pltpu.VMEM(params.shape, jnp.float32),
            pltpu.VMEM((2, padded), jnp.float32),
            pltpu.VMEM((2,) + field[1:], jnp.bfloat16),
            pltpu.VMEM((2, KERN * KERN, 16, LANE), jnp.bfloat16),
            pltpu.SemaphoreType.DMA((5,)),
            pltpu.SemaphoreType.DMA((blocks,)),
        ],
        32, x, expand_padded, kernel_padded, params, received,
    )


def lift_kernel(
    spread_hbm, param_hbm, w1_hbm, b1_hbm, w2_hbm, b2_hbm, wp_hbm, mean3_hbm, recv_hbm,
    proj_hbm, stat_ref, new_ref,
    recv_ref, lift_ref, param_ref, w1_ref, b1_ref, w2_ref, b2_ref, wp_ref, mean3_ref,
    coef_ref, pool_ref, gate_ref, scaled_ref, proj_ref, in_sems, sems, out_sems, *, layer, parts, row_count,
):
    blocks, cells = lift_ref.shape[0], lift_ref.shape[1]
    mid = w1_ref.shape[0]

    def enter(block):
        return pltpu.make_async_copy(spread_hbm.at[block], lift_ref.at[block], in_sems.at[block])

    copies = start_copies([(recv_hbm, recv_ref), (param_hbm, param_ref)], sems)
    for block in range(blocks):
        enter(block).start()
    pairs = [
        (w1_hbm.at[layer], w1_ref), (b1_hbm, b1_ref), (w2_hbm.at[layer], w2_ref), (b2_hbm, b2_ref),
        (wp_hbm.at[layer], wp_ref), (mean3_hbm, mean3_ref),
    ]
    weights = [pltpu.make_async_copy(source, target, sems.at[n + 2]) for n, (source, target) in enumerate(pairs)]
    for copy in weights:
        copy.start()
    for copy in copies:
        copy.wait()
    settle(recv_ref, param_ref, (2 * layer + 1, 0.5), coef_ref, new_ref, row_count)
    at = slice(layer, layer + 1)
    batch = 24

    def block_step(j, carry):
        here = pl.ds(pl.multiple_of(j * LANE, LANE), LANE)
        scale = coef_ref[0:1, here]
        shift = coef_ref[1:2, here]
        enter(j).wait()

        def step(i, pooled):
            cell = pl.multiple_of(i * batch, batch)
            lifted = half_silu(lift_ref[j, pl.ds(cell, batch)] * scale + shift)
            lift_ref[j, pl.ds(cell, batch)] = lifted
            return pooled + jnp.sum(lifted, axis=0)

        pooled = lax.fori_loop(0, cells // batch, step, jnp.zeros((16, LANE), jnp.float32))
        pool_ref[:, here] = pooled * (1.0 / cells)
        return carry

    lax.fori_loop(0, blocks, block_step, 0)
    for copy in weights:
        copy.wait()

    squeezed = b1_ref[at, :] + jnp.dot(
        pool_ref[:, :mid], w1_ref[...], precision=lax.Precision.HIGHEST, preferred_element_type=jnp.float32
    )
    squeezed = half_silu(0.5 * squeezed)
    grown = b2_ref[at, :] + jnp.dot(
        squeezed, w2_ref[...], precision=lax.Precision.HIGHEST, preferred_element_type=jnp.float32
    )
    gate_ref[:, :mid] = 0.5 + 0.5 * jnp.tanh(0.5 * grown)

    group = cells // parts
    out = proj_ref.shape[2]

    def leave(part):
        return pltpu.make_async_copy(proj_ref.at[part], proj_hbm.at[part], out_sems.at[part])

    def part_step(part, carry):
        first, second = carry
        base = pl.multiple_of(part * group, group)
        for k in range(blocks):
            size = min(LANE, mid - k * LANE)
            gate = gate_ref[:, k * LANE : k * LANE + size]
            scaled = (lift_ref[k, pl.ds(base, group), :, :size] * gate).reshape(group * 16, size)
            scaled_ref[:, k * LANE : k * LANE + size] = scaled.astype(jnp.bfloat16)
        projected = jnp.dot(scaled_ref[...], wp_ref[...], preferred_element_type=jnp.float32)
        proj_ref[part] = projected
        leave(part).start()
        centered = projected - mean3_ref[at, :]
        return first + fold_rows(centered), second + fold_rows(centered * centered)

    zero = jnp.zeros((8, out), jnp.float32)
    first, second = lax.fori_loop(0, parts, part_step, (zero, zero))
    stat_ref[...] = stat_copies(first, second, stat_ref.shape[0])
    for part in range(parts):
        leave(part).wait()


def lift_call(
    spread, params, squeeze_weight, squeeze_bias, excite_weight, excite_bias, project_weight, out_mean,
    received, members, layer, row_count,
):
    blocks, cells = spread.shape[:2]
    mid, out = project_weight.shape[1:]
    parts = 3
    rows = cells * 16
    return call(
        functools.partial(lift_kernel, layer=layer, parts=parts, row_count=row_count),
        "lift_project", (),
        [
            (jax.ShapeDtypeStruct((parts, rows // parts, out), jnp.float32), False),
            (jax.ShapeDtypeStruct((members, 2, out), jnp.float32), True),
            (jax.ShapeDtypeStruct((2, mid), jnp.float32), True),
        ],
        [
            pltpu.VMEM(received.shape, jnp.float32),
            pltpu.VMEM(spread.shape, jnp.float32),
            pltpu.VMEM(params.shape, jnp.float32),
            pltpu.VMEM(squeeze_weight.shape[1:], jnp.float32),
            pltpu.VMEM(squeeze_bias.shape, jnp.float32),
            pltpu.VMEM(excite_weight.shape[1:], jnp.float32),
            pltpu.VMEM(excite_bias.shape, jnp.float32),
            pltpu.VMEM(project_weight.shape[1:], project_weight.dtype),
            pltpu.VMEM(out_mean.shape, jnp.float32),
            pltpu.VMEM((2, blocks * LANE), jnp.float32),
            pltpu.VMEM((16, blocks * LANE), jnp.float32),
            pltpu.VMEM((16, blocks * LANE), jnp.float32),
            pltpu.VMEM((rows // parts, mid), jnp.bfloat16),
            pltpu.VMEM((parts, rows // parts, out), jnp.float32),
            pltpu.SemaphoreType.DMA((blocks,)),
            pltpu.SemaphoreType.DMA((8,)),
            pltpu.SemaphoreType.DMA((parts,)),
        ],
        40, spread, params, squeeze_weight, squeeze_bias, excite_weight, excite_bias, project_weight, out_mean,
        received,
    )


def output_kernel(x_hbm, proj_hbm, param_hbm, recv_hbm, *rest, layer, parts, row_count, follow):
    if follow:
        w_hbm, mid_mean_hbm, next_hbm, new_ref, stat_ref = rest[:5]
        w_ref, mid_mean_ref, in_sems, more_sems, out_sems = rest[10:]
        recv_ref, x_ref, proj_ref, param_ref, coef_ref = rest[5:10]
    else:
        next_hbm, new_ref, recv_ref, x_ref, proj_ref, param_ref, coef_ref, in_sems, out_sems = rest
    copies = start_copies([(recv_hbm, recv_ref), (param_hbm, param_ref), (x_hbm, x_ref)], in_sems)
    enter = [
        pltpu.make_async_copy(proj_hbm.at[part], proj_ref.at[part], in_sems.at[3 + part]) for part in range(parts)
    ]
    for copy in enter:
        copy.start()
    if follow:
        more = start_copies([(w_hbm.at[layer + 1], w_ref), (mid_mean_hbm.at[layer + 1], mid_mean_ref)], more_sems)
    for copy in copies[:2]:
        copy.wait()
    settle(recv_ref, param_ref, (layer, 1.0), coef_ref, new_ref, row_count)
    copies[2].wait()
    scale = coef_ref[0:1, :]
    shift = coef_ref[1:2, :]
    size = proj_ref.shape[1]
    leave = [
        pltpu.make_async_copy(
            x_ref.at[part * size : (part + 1) * size], next_hbm.at[part * size : (part + 1) * size], out_sems.at[part]
        )
        for part in range(parts)
    ]
    for part in range(parts):
        enter[part].wait()

        def step(i, carry):
            inner = pl.ds(pl.multiple_of(i * 192, 192), 192)
            here = pl.ds(pl.multiple_of(part * size + i * 192, 192), 192)
            total = x_ref[here, :].astype(jnp.float32) + proj_ref[part, inner, :] * scale + shift
            x_ref[here, :] = total.astype(jnp.bfloat16)
            return carry

        lax.fori_loop(0, size // 192, step, 0)
        leave[part].start()
    if follow:
        for copy in more:
            copy.wait()
        expand_moments(x_ref, w_ref, mid_mean_ref, stat_ref, 3)
    for copy in leave:
        copy.wait()


def output_call(x, projected, params, received, members, layer, row_count, follow=None):
    rows, out = x.shape
    parts = projected.shape[0]
    outs = [
        (jax.ShapeDtypeStruct((rows, out), jnp.bfloat16), False),
        (jax.ShapeDtypeStruct((2, out), jnp.float32), True),
    ]
    scratch = [
        pltpu.VMEM(received.shape, jnp.float32),
        pltpu.VMEM((rows, out), jnp.bfloat16),
        pltpu.VMEM(projected.shape, jnp.float32),
        pltpu.VMEM(params.shape, jnp.float32),
        pltpu.VMEM((2, out), jnp.float32),
    ]
    sems = [pltpu.SemaphoreType.DMA((3 + parts,)), pltpu.SemaphoreType.DMA((parts,))]
    operands = [x, projected, params, received]
    if follow is not None:
        mid = follow[0].shape[2]
        outs.append((jax.ShapeDtypeStruct((members, 2, mid), jnp.float32), True))
        scratch += [pltpu.VMEM((out, mid), jnp.bfloat16), pltpu.VMEM((2, mid), jnp.float32)]
        sems.insert(1, pltpu.SemaphoreType.DMA((2,)))
        operands += list(follow)
    return call(
        functools.partial(
            output_kernel, layer=layer, parts=parts, row_count=row_count, follow=follow is not None
        ),
        "block_output", (), outs, scratch + sems, 24, *operands,
    )


def exchange(stats):
    sums = lax.all_to_all(stats, "row", split_axis=0, concat_axis=0, tiled=True)
    total = jnp.sum(sums, axis=0)
    copies = jnp.broadcast_to(total[None], (lax.axis_size("col"),) + total.shape)
    return jnp.sum(lax.all_to_all(copies, "col", split_axis=0, concat_axis=0, tiled=True), axis=0)


def per_device(
    images, expand_weight, depth_kernel, squeeze_weight, squeeze_bias, excite_weight, excite_bias,
    project_weight, mid_gain, mid_bias, out_gain, out_bias, mid_mean, mid_var, out_mean, out_var,
):
    batch, side, _, out = images.shape
    mid = expand_weight.shape[2]
    members = lax.axis_size("row")
    row_count = float(batch * side * side * members * lax.axis_size("col"))
    spare = -mid % LANE
    widen = lambda a: jnp.pad(a, [(0, 0)] * (a.ndim - 1) + [(0, spare)])
    current = jnp.transpose(images, (1, 2, 0, 3)).reshape(side * side * batch, out)
    stats = moments_call(current, expand_weight, mid_mean, 0, members)
    expand_padded, kernel_padded = widen(expand_weight), widen(depth_kernel)
    params = jnp.stack([mid_mean, mid_var, mid_gain, mid_bias], axis=2)
    params = widen(params.reshape(LAYERS * 2 * 4, mid))
    out_params = jnp.stack([out_mean, out_var, out_gain, out_bias], axis=1).reshape(LAYERS * 4, out)
    mid_new, out_new = [], []
    for layer in range(LAYERS):
        spread, stats, first_new = depth_call(
            current, expand_padded, kernel_padded, params, exchange(stats), members, layer, side, row_count
        )
        projected, stats, second_new = lift_call(
            spread, params, squeeze_weight, squeeze_bias, excite_weight, excite_bias,
            project_weight, out_mean, exchange(stats), members, layer, row_count,
        )
        follow = (expand_weight, mid_mean) if layer + 1 < LAYERS else None
        results = output_call(current, projected, out_params, exchange(stats), members, layer, row_count, follow)
        current, third_new = results[0], results[1]
        if follow is not None:
            stats = results[2]
        mid_new.append(jnp.stack([first_new, second_new]))
        out_new.append(third_new)
    mid_new = jnp.stack(mid_new)
    out_new = jnp.stack(out_new)
    block_output = jnp.transpose(current.reshape(side, side, batch, out), (2, 0, 1, 3))
    return block_output, mid_new[:, :, 0], mid_new[:, :, 1], out_new[:, 0], out_new[:, 1]


def solution(mesh):
    split = P(("row", "col"), None, None, None)
    return jax.shard_map(
        per_device, mesh=mesh, in_specs=(split,) + (P(),) * 15, out_specs=(split, P(), P(), P(), P()), check_vma=False
    )
```

```python
import functools
import jax
import jax.numpy as jnp
from jax import lax
from jax.experimental import pallas as pl
from jax.experimental.pallas import tpu as pltpu
from jax.sharding import PartitionSpec as P

KERN = 5
LAYERS = 2
EPSILON = 0.001
RATIO_MAX = 3.0
SHIFT_MAX = 5.0
MOMENTUM = 0.01
LANE = 128
WIDE = 256
MIB = 1 << 20
GROUP = 1


def coefficients(received, row_count, run_mean, run_var, gain, bias):
    offset = received[0:1] / row_count
    batch_var = received[1:2] / row_count - offset * offset
    batch_mean = run_mean + offset
    batch_sigma = jnp.sqrt(batch_var + EPSILON)
    run_sigma = jnp.sqrt(run_var + EPSILON)
    scale_ratio = jnp.clip(batch_sigma / run_sigma, 1.0 / RATIO_MAX, RATIO_MAX)
    shift_clip = jnp.clip(offset / run_sigma, -SHIFT_MAX, SHIFT_MAX)
    gain_scale = gain * scale_ratio / batch_sigma
    gain_shift = bias + gain * shift_clip - batch_mean * gain_scale
    new_mean = run_mean + MOMENTUM * offset
    new_var = run_var + MOMENTUM * (batch_var - run_var)
    return gain_scale, gain_shift, new_mean, new_var


def settle(recv_ref, param_ref, at, coef_ref, new_ref, row_count):
    size = recv_ref.shape[1]
    coef_ref[...] = jnp.zeros(coef_ref.shape, jnp.float32)
    coef_ref[:, :size] = recv_ref[...]
    index, half = at
    mean, var, gain, bias = [param_ref[4 * index + n : 4 * index + n + 1, :] for n in range(4)]
    scale, shift, new_mean, new_var = coefficients(coef_ref[...], row_count, mean, var, gain, bias)
    coef_ref[...] = half * jnp.concatenate([scale, shift], axis=0)
    new_ref[...] = jnp.concatenate([new_mean, new_var], axis=0)[:, :size]


def start_copies(pairs, sems):
    copies = [pltpu.make_async_copy(source, target, sems.at[n]) for n, (source, target) in enumerate(pairs)]
    for copy in copies:
        copy.start()
    return copies


def half_silu(half):
    return half + half * jnp.tanh(half)


def fold_rows(block):
    return jnp.sum(block.reshape(block.shape[0] // 8, 8, block.shape[1]), axis=0)


def stat_copies(first, second, members):
    pair = jnp.concatenate(
        [jnp.sum(first, axis=0, keepdims=True), jnp.sum(second, axis=0, keepdims=True)], axis=0
    )
    return jnp.broadcast_to(pair[None], (members,) + pair.shape)


def call(kernel, name, in_vmem, outs, scratch, limit, *operands):
    spec = lambda inside: pl.BlockSpec(memory_space=pltpu.VMEM if inside else pltpu.HBM)
    return pl.pallas_call(
        kernel,
        in_specs=[spec(n in in_vmem) for n in range(len(operands))],
        out_specs=[spec(inside) for _, inside in outs],
        out_shape=[shape for shape, _ in outs],
        scratch_shapes=scratch,
        compiler_params=pltpu.CompilerParams(vmem_limit_bytes=62 * MIB),
        name=name,
    )(*operands)


def expand_moments(x_ref, w_ref, mean_ref, stat_ref, parts):
    rows = x_ref.shape[0]
    mid = w_ref.shape[1]
    chunk = rows // parts

    def lanes(here):
        mean = mean_ref[0:1, here]
        first = second = None
        for part in range(parts):
            values = jnp.dot(
                x_ref[part * chunk : (part + 1) * chunk, :], w_ref[:, here],
                preferred_element_type=jnp.float32,
            )
            centered = values - mean
            one, two = fold_rows(centered), fold_rows(centered * centered)
            first = one if first is None else first + one
            second = two if second is None else second + two
        stat_ref[:, :, here] = stat_copies(first, second, stat_ref.shape[0])

    def step(j, carry):
        lanes(pl.ds(pl.multiple_of(j * WIDE, WIDE), WIDE))
        return carry

    full = mid // WIDE
    lax.fori_loop(0, full, step, 0)
    if mid > full * WIDE:
        lanes(slice(full * WIDE, mid))


def moments_kernel(x_hbm, w_hbm, mean_hbm, stat_ref, x_ref, w_ref, mean_ref, sems, *, layer, parts):
    pairs = [(x_hbm, x_ref), (w_hbm.at[layer], w_ref), (mean_hbm.at[layer], mean_ref)]
    for copy in start_copies(pairs, sems):
        copy.wait()
    expand_moments(x_ref, w_ref, mean_ref, stat_ref, parts)


def moments_call(x, expand_weight, mid_mean, layer, members):
    _, out, mid = expand_weight.shape
    return call(
        functools.partial(moments_kernel, layer=layer, parts=3),
        "expand_moments", (),
        [(jax.ShapeDtypeStruct((members, 2, mid), jnp.float32), True)],
        [
            pltpu.VMEM(x.shape, x.dtype),
            pltpu.VMEM((out, mid), expand_weight.dtype),
            pltpu.VMEM((2, mid), jnp.float32),
            pltpu.SemaphoreType.DMA((3,)),
        ],
        20, x, expand_weight, mid_mean,
    )[0]


def depth_kernel_body(
    x_hbm, w_hbm, dk_hbm, param_hbm, recv_hbm, spread_hbm, stat_ref, new_ref,
    recv_ref, spread_ref, x_ref, w_ref, dk_ref, param_ref, coef_ref, act_ref, tap_ref, in_sems, out_sems,
    *, layer, side, parts, row_count,
):
    copies = start_copies(
        [
            (recv_hbm, recv_ref), (param_hbm, param_ref), (x_hbm, x_ref), (w_hbm.at[layer], w_ref),
            (dk_hbm.at[layer], dk_ref),
        ],
        in_sems,
    )
    for copy in copies[:2]:
        copy.wait()
    settle(recv_ref, param_ref, (2 * layer, 0.5), coef_ref, new_ref, row_count)
    for copy in copies[2:]:
        copy.wait()
    rows = x_ref.shape[0]
    mid = stat_ref.shape[2]
    blocks = spread_ref.shape[0]
    reach = KERN // 2
    chunk = rows // parts
    cells = chunk // 16

    def leave(block):
        return pltpu.make_async_copy(spread_ref.at[block], spread_hbm.at[block], out_sems.at[block])

    def activate(start, width):
        here = pl.ds(start, width)
        scale = coef_ref[0:1, here]
        shift = coef_ref[1:2, here]
        for part in range(parts):
            values = jnp.dot(
                x_ref[part * chunk : (part + 1) * chunk, :], w_ref[:, here],
                preferred_element_type=jnp.float32,
            )
            active = half_silu(values * scale + shift).astype(jnp.bfloat16).reshape(cells, 16, width)
            for s in range(width // LANE):
                act_ref[s, part * cells : (part + 1) * cells] = active[:, :, s * LANE : (s + 1) * LANE]

    def spread_block(s, block, start, size):
        here = pl.ds(start, LANE)
        mean = param_ref[8 * layer + 4 : 8 * layer + 5, here]
        for t in range(KERN * KERN):
            tap_ref[s, t] = jnp.broadcast_to(dk_ref[t : t + 1, here], (16, LANE)).astype(jnp.bfloat16)
        first = jnp.zeros((16, LANE), jnp.float32)
        second = jnp.zeros((16, LANE), jnp.float32)
        for h in range(side):
            for base in range(0, side, GROUP):
                group = range(base, base + GROUP)
                acc = {w: None for w in group}
                for i in range(KERN):
                    r = h + i - reach
                    if not 0 <= r < side:
                        continue
                    for p in range(max(0, base - reach), min(side, base + GROUP + reach)):
                        cell = act_ref[s, r * side + p].astype(jnp.float32)
                        for w in group:
                            k = p - w + reach
                            if 0 <= k < KERN:
                                term = cell * tap_ref[s, i * KERN + k].astype(jnp.float32)
                                acc[w] = term if acc[w] is None else acc[w] + term
                for w in group:
                    spread_ref[block, h * side + w] = acc[w].astype(spread_ref.dtype)
                    centered = acc[w] - mean
                    first = first + centered
                    second = second + centered * centered
        copies = stat_copies(first, second, stat_ref.shape[0])
        stat_ref[:, :, pl.ds(start, size)] = copies[:, :, :size]
        leave(block).start()

    def step(j, carry):
        start = pl.multiple_of(j * WIDE, WIDE)
        activate(start, WIDE)
        spread_block(0, 2 * j, start, LANE)
        spread_block(1, 2 * j + 1, pl.multiple_of(start + LANE, LANE), LANE)
        return carry

    lax.fori_loop(0, blocks // 2, step, 0)
    if blocks % 2:
        start = (blocks - 1) * LANE
        activate(start, LANE)
        spread_block(0, blocks - 1, start, mid - start)
    for block in range(blocks):
        leave(block).wait()


def depth_call(x, expand_padded, kernel_padded, params, received, members, layer, side, row_count):
    _, out, padded = expand_padded.shape
    mid = received.shape[1]
    blocks = padded // LANE
    field = (blocks, side * side, 16, LANE)
    return call(
        functools.partial(depth_kernel_body, layer=layer, side=side, parts=3, row_count=row_count),
        "depthwise", (),
        [
            (jax.ShapeDtypeStruct(field, jnp.bfloat16), False),
            (jax.ShapeDtypeStruct((members, 2, mid), jnp.float32), True),
            (jax.ShapeDtypeStruct((2, mid), jnp.float32), True),
        ],
        [
            pltpu.VMEM(received.shape, jnp.float32),
            pltpu.VMEM(field, jnp.bfloat16),
            pltpu.VMEM(x.shape, x.dtype),
            pltpu.VMEM((out, padded), expand_padded.dtype),
            pltpu.VMEM(kernel_padded.shape[1:], jnp.float32),
            pltpu.VMEM(params.shape, jnp.float32),
            pltpu.VMEM((2, padded), jnp.float32),
            pltpu.VMEM((2,) + field[1:], jnp.bfloat16),
            pltpu.VMEM((2, KERN * KERN, 16, LANE), jnp.bfloat16),
            pltpu.SemaphoreType.DMA((5,)),
            pltpu.SemaphoreType.DMA((blocks,)),
        ],
        32, x, expand_padded, kernel_padded, params, received,
    )


def lift_kernel(
    spread_hbm, param_hbm, w1_hbm, b1_hbm, w2_hbm, b2_hbm, wp_hbm, mean3_hbm, recv_hbm,
    proj_hbm, stat_ref, new_ref,
    recv_ref, spread_ref, lift_ref, param_ref, w1_ref, b1_ref, w2_ref, b2_ref, wp_ref, mean3_ref,
    coef_ref, pool_ref, gate_ref, scaled_ref, proj_ref, in_sems, sems, out_sems, *, layer, parts, row_count,
):
    blocks, cells = lift_ref.shape[0], lift_ref.shape[1]
    mid = w1_ref.shape[0]

    def enter(block):
        return pltpu.make_async_copy(spread_hbm.at[block], spread_ref.at[block], in_sems.at[block])

    copies = start_copies([(recv_hbm, recv_ref), (param_hbm, param_ref)], sems)
    for block in range(blocks):
        enter(block).start()
    pairs = [
        (w1_hbm.at[layer], w1_ref), (b1_hbm, b1_ref), (w2_hbm.at[layer], w2_ref), (b2_hbm, b2_ref),
        (wp_hbm.at[layer], wp_ref), (mean3_hbm, mean3_ref),
    ]
    weights = [pltpu.make_async_copy(source, target, sems.at[n + 2]) for n, (source, target) in enumerate(pairs)]
    for copy in weights:
        copy.start()
    for copy in copies:
        copy.wait()
    settle(recv_ref, param_ref, (2 * layer + 1, 0.5), coef_ref, new_ref, row_count)
    at = slice(layer, layer + 1)
    batch = 24

    def block_step(j, carry):
        here = pl.ds(pl.multiple_of(j * LANE, LANE), LANE)
        scale = coef_ref[0:1, here]
        shift = coef_ref[1:2, here]
        enter(j).wait()

        def step(i, pooled):
            cell = pl.multiple_of(i * batch, batch)
            lifted = half_silu(spread_ref[j, pl.ds(cell, batch)].astype(jnp.float32) * scale + shift)
            lift_ref[j, pl.ds(cell, batch)] = lifted
            return pooled + jnp.sum(lifted, axis=0)

        pooled = lax.fori_loop(0, cells // batch, step, jnp.zeros((16, LANE), jnp.float32))
        pool_ref[:, here] = pooled * (1.0 / cells)
        return carry

    lax.fori_loop(0, blocks, block_step, 0)
    for copy in weights:
        copy.wait()

    squeezed = b1_ref[at, :] + jnp.dot(
        pool_ref[:, :mid], w1_ref[...], precision=lax.Precision.HIGHEST, preferred_element_type=jnp.float32
    )
    squeezed = half_silu(0.5 * squeezed)
    grown = b2_ref[at, :] + jnp.dot(
        squeezed, w2_ref[...], precision=lax.Precision.HIGHEST, preferred_element_type=jnp.float32
    )
    gate_ref[:, :mid] = 0.5 + 0.5 * jnp.tanh(0.5 * grown)

    group = cells // parts
    out = proj_ref.shape[2]

    def leave(part):
        return pltpu.make_async_copy(proj_ref.at[part], proj_hbm.at[part], out_sems.at[part])

    def part_step(part, carry):
        first, second = carry
        base = pl.multiple_of(part * group, group)
        for k in range(blocks):
            size = min(LANE, mid - k * LANE)
            gate = gate_ref[:, k * LANE : k * LANE + size]
            scaled = (lift_ref[k, pl.ds(base, group), :, :size] * gate).reshape(group * 16, size)
            scaled_ref[:, k * LANE : k * LANE + size] = scaled.astype(jnp.bfloat16)
        projected = jnp.dot(scaled_ref[...], wp_ref[...], preferred_element_type=jnp.float32)
        proj_ref[part] = projected
        leave(part).start()
        centered = projected - mean3_ref[at, :]
        return first + fold_rows(centered), second + fold_rows(centered * centered)

    zero = jnp.zeros((8, out), jnp.float32)
    first, second = lax.fori_loop(0, parts, part_step, (zero, zero))
    stat_ref[...] = stat_copies(first, second, stat_ref.shape[0])
    for part in range(parts):
        leave(part).wait()


def lift_call(
    spread, params, squeeze_weight, squeeze_bias, excite_weight, excite_bias, project_weight, out_mean,
    received, members, layer, row_count,
):
    blocks, cells = spread.shape[:2]
    mid, out = project_weight.shape[1:]
    parts = 3
    rows = cells * 16
    return call(
        functools.partial(lift_kernel, layer=layer, parts=parts, row_count=row_count),
        "lift_project", (),
        [
            (jax.ShapeDtypeStruct((parts, rows // parts, out), jnp.float32), False),
            (jax.ShapeDtypeStruct((members, 2, out), jnp.float32), True),
            (jax.ShapeDtypeStruct((2, mid), jnp.float32), True),
        ],
        [
            pltpu.VMEM(received.shape, jnp.float32),
            pltpu.VMEM(spread.shape, spread.dtype),
            pltpu.VMEM(spread.shape, jnp.float32),
            pltpu.VMEM(params.shape, jnp.float32),
            pltpu.VMEM(squeeze_weight.shape[1:], jnp.float32),
            pltpu.VMEM(squeeze_bias.shape, jnp.float32),
            pltpu.VMEM(excite_weight.shape[1:], jnp.float32),
            pltpu.VMEM(excite_bias.shape, jnp.float32),
            pltpu.VMEM(project_weight.shape[1:], project_weight.dtype),
            pltpu.VMEM(out_mean.shape, jnp.float32),
            pltpu.VMEM((2, blocks * LANE), jnp.float32),
            pltpu.VMEM((16, blocks * LANE), jnp.float32),
            pltpu.VMEM((16, blocks * LANE), jnp.float32),
            pltpu.VMEM((rows // parts, mid), jnp.bfloat16),
            pltpu.VMEM((parts, rows // parts, out), jnp.float32),
            pltpu.SemaphoreType.DMA((blocks,)),
            pltpu.SemaphoreType.DMA((8,)),
            pltpu.SemaphoreType.DMA((parts,)),
        ],
        40, spread, params, squeeze_weight, squeeze_bias, excite_weight, excite_bias, project_weight, out_mean,
        received,
    )


def output_kernel(x_hbm, proj_hbm, param_hbm, recv_hbm, *rest, layer, parts, row_count, follow):
    if follow:
        w_hbm, mid_mean_hbm, next_hbm, new_ref, stat_ref = rest[:5]
        w_ref, mid_mean_ref, in_sems, more_sems, out_sems = rest[10:]
        recv_ref, x_ref, proj_ref, param_ref, coef_ref = rest[5:10]
    else:
        earlier_ref, next_hbm, means_ref, vars_ref, new_ref, recv_ref, x_ref, proj_ref = rest[:8]
        param_ref, coef_ref, in_sems, out_sems = rest[8:]
    copies = start_copies([(recv_hbm, recv_ref), (param_hbm, param_ref), (x_hbm, x_ref)], in_sems)
    enter = [
        pltpu.make_async_copy(proj_hbm.at[part], proj_ref.at[part], in_sems.at[3 + part]) for part in range(parts)
    ]
    for copy in enter:
        copy.start()
    if follow:
        more = start_copies([(w_hbm.at[layer + 1], w_ref), (mid_mean_hbm.at[layer + 1], mid_mean_ref)], more_sems)
    for copy in copies[:2]:
        copy.wait()
    settle(recv_ref, param_ref, (layer, 1.0), coef_ref, new_ref, row_count)
    copies[2].wait()
    scale = coef_ref[0:1, :]
    shift = coef_ref[1:2, :]
    size = proj_ref.shape[1]
    leave = [
        pltpu.make_async_copy(
            x_ref.at[part * size : (part + 1) * size], next_hbm.at[part * size : (part + 1) * size], out_sems.at[part]
        )
        for part in range(parts)
    ]
    for part in range(parts):
        enter[part].wait()

        def step(i, carry):
            inner = pl.ds(pl.multiple_of(i * 192, 192), 192)
            here = pl.ds(pl.multiple_of(part * size + i * 192, 192), 192)
            total = x_ref[here, :].astype(jnp.float32) + proj_ref[part, inner, :] * scale + shift
            x_ref[here, :] = total.astype(jnp.bfloat16)
            return carry

        lax.fori_loop(0, size // 192, step, 0)
        leave[part].start()
    if not follow:
        means_ref[:layer] = earlier_ref[0]
        means_ref[layer:] = new_ref[0:1]
        vars_ref[:layer] = earlier_ref[1]
        vars_ref[layer:] = new_ref[1:2]
    if follow:
        for copy in more:
            copy.wait()
        expand_moments(x_ref, w_ref, mid_mean_ref, stat_ref, 3)
    for copy in leave:
        copy.wait()


def output_call(x, projected, params, received, members, layer, row_count, follow=None, earlier=None):
    rows, out = x.shape
    parts = projected.shape[0]
    outs = [(jax.ShapeDtypeStruct((rows, out), jnp.bfloat16), False)]
    scratch = [
        pltpu.VMEM(received.shape, jnp.float32),
        pltpu.VMEM((rows, out), jnp.bfloat16),
        pltpu.VMEM(projected.shape, jnp.float32),
        pltpu.VMEM(params.shape, jnp.float32),
        pltpu.VMEM((2, out), jnp.float32),
    ]
    sems = [pltpu.SemaphoreType.DMA((3 + parts,)), pltpu.SemaphoreType.DMA((parts,))]
    operands = [x, projected, params, received]
    if follow is not None:
        mid = follow[0].shape[2]
        outs.append((jax.ShapeDtypeStruct((2, out), jnp.float32), True))
        outs.append((jax.ShapeDtypeStruct((members, 2, mid), jnp.float32), True))
        scratch += [pltpu.VMEM((out, mid), jnp.bfloat16), pltpu.VMEM((2, mid), jnp.float32)]
        sems.insert(1, pltpu.SemaphoreType.DMA((2,)))
        operands += list(follow)
        inside = ()
    else:
        outs += [(jax.ShapeDtypeStruct((LAYERS, out), jnp.float32), True)] * 2
        scratch.insert(0, pltpu.VMEM((2, out), jnp.float32))
        operands.append(earlier)
        inside = (4,)
    return call(
        functools.partial(
            output_kernel, layer=layer, parts=parts, row_count=row_count, follow=follow is not None
        ),
        "block_output", inside, outs, scratch + sems, 24, *operands,
    )


def exchange(stats):
    sums = lax.all_to_all(stats, "row", split_axis=0, concat_axis=0, tiled=True)
    total = jnp.sum(sums, axis=0)
    copies = jnp.broadcast_to(total[None], (lax.axis_size("col"),) + total.shape)
    return jnp.sum(lax.all_to_all(copies, "col", split_axis=0, concat_axis=0, tiled=True), axis=0)


def per_device(
    images, expand_weight, depth_kernel, squeeze_weight, squeeze_bias, excite_weight, excite_bias,
    project_weight, mid_gain, mid_bias, out_gain, out_bias, mid_mean, mid_var, out_mean, out_var,
):
    batch, side, _, out = images.shape
    mid = expand_weight.shape[2]
    members = lax.axis_size("row")
    row_count = float(batch * side * side * members * lax.axis_size("col"))
    spare = -mid % LANE
    widen = lambda a: jnp.pad(a, [(0, 0)] * (a.ndim - 1) + [(0, spare)])
    current = jnp.transpose(images, (1, 2, 0, 3)).reshape(side * side * batch, out)
    stats = moments_call(current, expand_weight, mid_mean, 0, members)
    expand_padded, kernel_padded = widen(expand_weight), widen(depth_kernel)
    params = jnp.stack([mid_mean, mid_var, mid_gain, mid_bias], axis=2)
    params = widen(params.reshape(LAYERS * 2 * 4, mid))
    out_params = jnp.stack([out_mean, out_var, out_gain, out_bias], axis=1).reshape(LAYERS * 4, out)
    mid_new, out_new = [], []
    for layer in range(LAYERS):
        spread, stats, first_new = depth_call(
            current, expand_padded, kernel_padded, params, exchange(stats), members, layer, side, row_count
        )
        projected, stats, second_new = lift_call(
            spread, params, squeeze_weight, squeeze_bias, excite_weight, excite_bias,
            project_weight, out_mean, exchange(stats), members, layer, row_count,
        )
        received = exchange(stats)
        if layer + 1 < LAYERS:
            current, third_new, stats = output_call(
                current, projected, out_params, received, members, layer, row_count, (expand_weight, mid_mean)
            )
            out_new.append(third_new)
        else:
            earlier = jnp.stack(out_new, axis=1)
            current, out_mean_new, out_var_new = output_call(
                current, projected, out_params, received, members, layer, row_count, None, earlier
            )
        mid_new.append(jnp.stack([first_new, second_new]))
    mid_new = jnp.stack(mid_new)
    block_output = jnp.transpose(current.reshape(side, side, batch, out), (2, 0, 1, 3))
    return block_output, mid_new[:, :, 0], mid_new[:, :, 1], out_mean_new, out_var_new


def solution(mesh):
    split = P(("row", "col"), None, None, None)
    return jax.shard_map(
        per_device, mesh=mesh, in_specs=(split,) + (P(),) * 15, out_specs=(split, P(), P(), P(), P()), check_vma=False
    )
```

```python
import functools
import jax
import jax.numpy as jnp
from jax import lax
from jax.experimental import pallas as pl
from jax.experimental.pallas import tpu as pltpu
from jax.sharding import PartitionSpec as P

KERN = 5
LAYERS = 2
EPSILON = 0.001
RATIO_MAX = 3.0
SHIFT_MAX = 5.0
MOMENTUM = 0.01
LANE = 128
WIDE = 256
MIB = 1 << 20


def coefficients(received, row_count, run_mean, run_var, gain, bias):
    offset = received[0:1] / row_count
    batch_var = received[1:2] / row_count - offset * offset
    batch_mean = run_mean + offset
    batch_sigma = jnp.sqrt(batch_var + EPSILON)
    run_sigma = jnp.sqrt(run_var + EPSILON)
    scale_ratio = jnp.clip(batch_sigma / run_sigma, 1.0 / RATIO_MAX, RATIO_MAX)
    shift_clip = jnp.clip(offset / run_sigma, -SHIFT_MAX, SHIFT_MAX)
    gain_scale = gain * scale_ratio / batch_sigma
    gain_shift = bias + gain * shift_clip - batch_mean * gain_scale
    new_mean = run_mean + MOMENTUM * offset
    new_var = run_var + MOMENTUM * (batch_var - run_var)
    return gain_scale, gain_shift, new_mean, new_var


def settle(recv_ref, param_ref, at, coef_ref, new_ref, row_count):
    size = recv_ref.shape[1]
    coef_ref[...] = jnp.zeros(coef_ref.shape, jnp.float32)
    coef_ref[:, :size] = recv_ref[...]
    index, half = at
    mean, var, gain, bias = [param_ref[4 * index + n : 4 * index + n + 1, :] for n in range(4)]
    scale, shift, new_mean, new_var = coefficients(coef_ref[...], row_count, mean, var, gain, bias)
    coef_ref[...] = half * jnp.concatenate([scale, shift], axis=0)
    new_ref[...] = jnp.concatenate([new_mean, new_var], axis=0)[:, :size]


def start_copies(pairs, sems):
    copies = [pltpu.make_async_copy(source, target, sems.at[n]) for n, (source, target) in enumerate(pairs)]
    for copy in copies:
        copy.start()
    return copies


def half_silu(half):
    return half + half * jnp.tanh(half)


def fold_rows(block):
    return jnp.sum(block.reshape(block.shape[0] // 8, 8, block.shape[1]), axis=0)


def stat_copies(first, second, members):
    pair = jnp.concatenate(
        [jnp.sum(first, axis=0, keepdims=True), jnp.sum(second, axis=0, keepdims=True)], axis=0
    )
    return jnp.broadcast_to(pair[None], (members,) + pair.shape)


def call(kernel, name, in_vmem, outs, scratch, limit, *operands):
    spec = lambda inside: pl.BlockSpec(memory_space=pltpu.VMEM if inside else pltpu.HBM)
    return pl.pallas_call(
        kernel,
        in_specs=[spec(n in in_vmem) for n in range(len(operands))],
        out_specs=[spec(inside) for _, inside in outs],
        out_shape=[shape for shape, _ in outs],
        scratch_shapes=scratch,
        compiler_params=pltpu.CompilerParams(vmem_limit_bytes=62 * MIB),
        name=name,
    )(*operands)


def expand_moments(x_ref, w_ref, mean_ref, stat_ref, parts):
    rows = x_ref.shape[0]
    mid = w_ref.shape[1]
    chunk = rows // parts

    def lanes(here):
        mean = mean_ref[0:1, here]
        first = second = None
        for part in range(parts):
            values = jnp.dot(
                x_ref[part * chunk : (part + 1) * chunk, :], w_ref[:, here],
                preferred_element_type=jnp.float32,
            )
            centered = values - mean
            one, two = fold_rows(centered), fold_rows(centered * centered)
            first = one if first is None else first + one
            second = two if second is None else second + two
        stat_ref[:, :, here] = stat_copies(first, second, stat_ref.shape[0])

    def step(j, carry):
        lanes(pl.ds(pl.multiple_of(j * WIDE, WIDE), WIDE))
        return carry

    full = mid // WIDE
    lax.fori_loop(0, full, step, 0)
    if mid > full * WIDE:
        lanes(slice(full * WIDE, mid))


def moments_kernel(x_hbm, w_hbm, mean_hbm, stat_ref, x_ref, w_ref, mean_ref, sems, *, layer, parts):
    pairs = [(x_hbm, x_ref), (w_hbm.at[layer], w_ref), (mean_hbm.at[layer], mean_ref)]
    for copy in start_copies(pairs, sems):
        copy.wait()
    expand_moments(x_ref, w_ref, mean_ref, stat_ref, parts)


def moments_call(x, expand_weight, mid_mean, layer, members):
    _, out, mid = expand_weight.shape
    return call(
        functools.partial(moments_kernel, layer=layer, parts=3),
        "expand_moments", (),
        [(jax.ShapeDtypeStruct((members, 2, mid), jnp.float32), True)],
        [
            pltpu.VMEM(x.shape, x.dtype),
            pltpu.VMEM((out, mid), expand_weight.dtype),
            pltpu.VMEM((2, mid), jnp.float32),
            pltpu.SemaphoreType.DMA((3,)),
        ],
        20, x, expand_weight, mid_mean,
    )[0]


def depth_kernel_body(
    x_ref, w_ref, dk_ref, recv_ref, param_ref, spread_ref, stat_ref, new_ref, act_ref, tap_ref,
    *, layer, row_count, side, parts, tail,
):
    j = pl.program_id(0)
    rows = x_ref.shape[0]
    reach = KERN // 2
    mean, var, gain, bias = [param_ref[8 * layer + n : 8 * layer + n + 1, :] for n in range(4)]
    scale, shift, new_mean, new_var = coefficients(recv_ref[...], row_count, mean, var, gain, bias)
    new_ref[...] = jnp.concatenate([new_mean, new_var], axis=0)
    scale = 0.5 * scale
    shift = 0.5 * shift
    chunk = rows // parts
    cells = chunk // 16
    for part in range(parts):
        values = jnp.dot(
            x_ref[part * chunk : (part + 1) * chunk, :], w_ref[0], preferred_element_type=jnp.float32
        )
        active = half_silu(values * scale + shift).astype(jnp.bfloat16).reshape(cells, 16, WIDE)
        for s in range(2):
            act_ref[s, part * cells : (part + 1) * cells] = active[:, :, s * LANE : (s + 1) * LANE]

    def lanes(s):
        here = slice(s * LANE, (s + 1) * LANE)
        mean = param_ref[8 * layer + 4 : 8 * layer + 5, here]
        for t in range(KERN * KERN):
            tap_ref[s, t] = jnp.broadcast_to(dk_ref[0, t : t + 1, here], (16, LANE)).astype(jnp.bfloat16)
        first = jnp.zeros((16, LANE), jnp.float32)
        second = jnp.zeros((16, LANE), jnp.float32)
        for h in range(side):
            for w in range(side):
                acc = None
                for i in range(KERN):
                    for k in range(KERN):
                        r, p = h + i - reach, w + k - reach
                        if 0 <= r < side and 0 <= p < side:
                            cell = act_ref[s, r * side + p].astype(jnp.float32)
                            term = cell * tap_ref[s, i * KERN + k].astype(jnp.float32)
                            acc = term if acc is None else acc + term
                spread_ref[s, h * side + w] = acc.astype(spread_ref.dtype)
                centered = acc - mean
                first = first + centered
                second = second + centered * centered
        pair = jnp.concatenate(
            [jnp.sum(first, axis=0, keepdims=True), jnp.sum(second, axis=0, keepdims=True)], axis=0
        )
        stat_ref[:, :, here] = jnp.broadcast_to(pair[None], (stat_ref.shape[0],) + pair.shape)

    lanes(0)
    if tail > LANE:
        lanes(1)
    else:
        pl.when(j < pl.num_programs(0) - 1)(lambda: lanes(1))


def depth_call(x, expand_weight, depth_kernel, params, received, members, layer, side, row_count):
    rows, out = x.shape
    mid = expand_weight.shape[2]
    cells = side * side
    steps = pl.cdiv(mid, WIDE)
    return pl.pallas_call(
        functools.partial(
            depth_kernel_body, layer=layer, row_count=row_count, side=side, parts=3, tail=mid - (steps - 1) * WIDE
        ),
        grid=(steps,),
        in_specs=[
            pl.BlockSpec((rows, out), lambda j: (0, 0)),
            pl.BlockSpec((1, out, WIDE), lambda j: (layer, 0, j)),
            pl.BlockSpec((1, KERN * KERN, WIDE), lambda j: (layer, 0, j)),
            pl.BlockSpec((2, WIDE), lambda j: (0, j)),
            pl.BlockSpec((params.shape[0], WIDE), lambda j: (0, j)),
        ],
        out_specs=[
            pl.BlockSpec((2, cells, 16, LANE), lambda j: (j, 0, 0, 0)),
            pl.BlockSpec((members, 2, WIDE), lambda j: (0, 0, j)),
            pl.BlockSpec((2, WIDE), lambda j: (0, j)),
        ],
        out_shape=[
            jax.ShapeDtypeStruct((pl.cdiv(mid, LANE), cells, 16, LANE), jnp.bfloat16),
            jax.ShapeDtypeStruct((members, 2, mid), jnp.float32),
            jax.ShapeDtypeStruct((2, mid), jnp.float32),
        ],
        scratch_shapes=[
            pltpu.VMEM((2, cells, 16, LANE), jnp.bfloat16),
            pltpu.VMEM((2, KERN * KERN, 16, LANE), jnp.bfloat16),
        ],
        compiler_params=pltpu.CompilerParams(vmem_limit_bytes=62 * MIB),
        name="depthwise",
    )(x, expand_weight, depth_kernel, received, params)


def lift_kernel(
    spread_hbm, param_hbm, w1_hbm, b1_hbm, w2_hbm, b2_hbm, wp_hbm, mean3_hbm, recv_hbm,
    proj_hbm, stat_ref, new_ref,
    recv_ref, spread_ref, lift_ref, param_ref, w1_ref, b1_ref, w2_ref, b2_ref, wp_ref, mean3_ref,
    coef_ref, pool_ref, gate_ref, scaled_ref, proj_ref, in_sems, sems, out_sems, *, layer, parts, row_count,
):
    blocks, cells = lift_ref.shape[0], lift_ref.shape[1]
    mid = w1_ref.shape[0]

    def enter(block):
        return pltpu.make_async_copy(spread_hbm.at[block], spread_ref.at[block], in_sems.at[block])

    copies = start_copies([(recv_hbm, recv_ref), (param_hbm, param_ref)], sems)
    for block in range(blocks):
        enter(block).start()
    pairs = [
        (w1_hbm.at[layer], w1_ref), (b1_hbm, b1_ref), (w2_hbm.at[layer], w2_ref), (b2_hbm, b2_ref),
        (wp_hbm.at[layer], wp_ref), (mean3_hbm, mean3_ref),
    ]
    weights = [pltpu.make_async_copy(source, target, sems.at[n + 2]) for n, (source, target) in enumerate(pairs)]
    for copy in weights:
        copy.start()
    for copy in copies:
        copy.wait()
    settle(recv_ref, param_ref, (2 * layer + 1, 0.5), coef_ref, new_ref, row_count)
    at = slice(layer, layer + 1)
    batch = 24

    def block_step(j, carry):
        here = pl.ds(pl.multiple_of(j * LANE, LANE), LANE)
        scale = coef_ref[0:1, here]
        shift = coef_ref[1:2, here]
        enter(j).wait()

        def step(i, pooled):
            cell = pl.multiple_of(i * batch, batch)
            lifted = half_silu(spread_ref[j, pl.ds(cell, batch)].astype(jnp.float32) * scale + shift)
            lift_ref[j, pl.ds(cell, batch)] = lifted
            return pooled + jnp.sum(lifted, axis=0)

        pooled = lax.fori_loop(0, cells // batch, step, jnp.zeros((16, LANE), jnp.float32))
        pool_ref[:, here] = pooled * (1.0 / cells)
        return carry

    lax.fori_loop(0, blocks, block_step, 0)
    for copy in weights:
        copy.wait()

    squeezed = b1_ref[at, :] + jnp.dot(
        pool_ref[:, :mid], w1_ref[...], precision=lax.Precision.HIGHEST, preferred_element_type=jnp.float32
    )
    squeezed = half_silu(0.5 * squeezed)
    grown = b2_ref[at, :] + jnp.dot(
        squeezed, w2_ref[...], precision=lax.Precision.HIGHEST, preferred_element_type=jnp.float32
    )
    gate_ref[:, :mid] = 0.5 + 0.5 * jnp.tanh(0.5 * grown)

    group = cells // parts
    out = proj_ref.shape[2]

    def leave(part):
        return pltpu.make_async_copy(proj_ref.at[part], proj_hbm.at[part], out_sems.at[part])

    def part_step(part, carry):
        first, second = carry
        base = pl.multiple_of(part * group, group)
        for k in range(blocks):
            size = min(LANE, mid - k * LANE)
            gate = gate_ref[:, k * LANE : k * LANE + size]
            scaled = (lift_ref[k, pl.ds(base, group), :, :size] * gate).reshape(group * 16, size)
            scaled_ref[:, k * LANE : k * LANE + size] = scaled.astype(jnp.bfloat16)
        projected = jnp.dot(scaled_ref[...], wp_ref[...], preferred_element_type=jnp.float32)
        proj_ref[part] = projected
        leave(part).start()
        centered = projected - mean3_ref[at, :]
        return first + fold_rows(centered), second + fold_rows(centered * centered)

    zero = jnp.zeros((8, out), jnp.float32)
    first, second = lax.fori_loop(0, parts, part_step, (zero, zero))
    stat_ref[...] = stat_copies(first, second, stat_ref.shape[0])
    for part in range(parts):
        leave(part).wait()


def lift_call(
    spread, params, squeeze_weight, squeeze_bias, excite_weight, excite_bias, project_weight, out_mean,
    received, members, layer, row_count,
):
    blocks, cells = spread.shape[:2]
    mid, out = project_weight.shape[1:]
    parts = 3
    rows = cells * 16
    return call(
        functools.partial(lift_kernel, layer=layer, parts=parts, row_count=row_count),
        "lift_project", (),
        [
            (jax.ShapeDtypeStruct((parts, rows // parts, out), jnp.float32), False),
            (jax.ShapeDtypeStruct((members, 2, out), jnp.float32), True),
            (jax.ShapeDtypeStruct((2, mid), jnp.float32), True),
        ],
        [
            pltpu.VMEM(received.shape, jnp.float32),
            pltpu.VMEM(spread.shape, spread.dtype),
            pltpu.VMEM(spread.shape, jnp.float32),
            pltpu.VMEM(params.shape, jnp.float32),
            pltpu.VMEM(squeeze_weight.shape[1:], jnp.float32),
            pltpu.VMEM(squeeze_bias.shape, jnp.float32),
            pltpu.VMEM(excite_weight.shape[1:], jnp.float32),
            pltpu.VMEM(excite_bias.shape, jnp.float32),
            pltpu.VMEM(project_weight.shape[1:], project_weight.dtype),
            pltpu.VMEM(out_mean.shape, jnp.float32),
            pltpu.VMEM((2, blocks * LANE), jnp.float32),
            pltpu.VMEM((16, blocks * LANE), jnp.float32),
            pltpu.VMEM((16, blocks * LANE), jnp.float32),
            pltpu.VMEM((rows // parts, mid), jnp.bfloat16),
            pltpu.VMEM((parts, rows // parts, out), jnp.float32),
            pltpu.SemaphoreType.DMA((blocks,)),
            pltpu.SemaphoreType.DMA((8,)),
            pltpu.SemaphoreType.DMA((parts,)),
        ],
        40, spread, params, squeeze_weight, squeeze_bias, excite_weight, excite_bias, project_weight, out_mean,
        received,
    )


def output_kernel(x_hbm, proj_hbm, param_hbm, recv_hbm, *rest, layer, parts, row_count, follow):
    if follow:
        w_hbm, mid_mean_hbm, next_hbm, new_ref, stat_ref = rest[:5]
        w_ref, mid_mean_ref, in_sems, more_sems, out_sems = rest[10:]
        recv_ref, x_ref, proj_ref, param_ref, coef_ref = rest[5:10]
    else:
        earlier_ref, next_hbm, means_ref, vars_ref, new_ref, recv_ref, x_ref, proj_ref = rest[:8]
        param_ref, coef_ref, in_sems, out_sems = rest[8:]
    copies = start_copies([(recv_hbm, recv_ref), (param_hbm, param_ref), (x_hbm, x_ref)], in_sems)
    enter = [
        pltpu.make_async_copy(proj_hbm.at[part], proj_ref.at[part], in_sems.at[3 + part]) for part in range(parts)
    ]
    for copy in enter:
        copy.start()
    if follow:
        more = start_copies([(w_hbm.at[layer + 1], w_ref), (mid_mean_hbm.at[layer + 1], mid_mean_ref)], more_sems)
    for copy in copies[:2]:
        copy.wait()
    settle(recv_ref, param_ref, (layer, 1.0), coef_ref, new_ref, row_count)
    copies[2].wait()
    scale = coef_ref[0:1, :]
    shift = coef_ref[1:2, :]
    size = proj_ref.shape[1]
    leave = [
        pltpu.make_async_copy(
            x_ref.at[part * size : (part + 1) * size], next_hbm.at[part * size : (part + 1) * size], out_sems.at[part]
        )
        for part in range(parts)
    ]
    for part in range(parts):
        enter[part].wait()

        def step(i, carry):
            inner = pl.ds(pl.multiple_of(i * 192, 192), 192)
            here = pl.ds(pl.multiple_of(part * size + i * 192, 192), 192)
            total = x_ref[here, :].astype(jnp.float32) + proj_ref[part, inner, :] * scale + shift
            x_ref[here, :] = total.astype(jnp.bfloat16)
            return carry

        lax.fori_loop(0, size // 192, step, 0)
        leave[part].start()
    if not follow:
        means_ref[:layer] = earlier_ref[0]
        means_ref[layer:] = new_ref[0:1]
        vars_ref[:layer] = earlier_ref[1]
        vars_ref[layer:] = new_ref[1:2]
    if follow:
        for copy in more:
            copy.wait()
        expand_moments(x_ref, w_ref, mid_mean_ref, stat_ref, 3)
    for copy in leave:
        copy.wait()


def output_call(x, projected, params, received, members, layer, row_count, follow=None, earlier=None):
    rows, out = x.shape
    parts = projected.shape[0]
    outs = [(jax.ShapeDtypeStruct((rows, out), jnp.bfloat16), False)]
    scratch = [
        pltpu.VMEM(received.shape, jnp.float32),
        pltpu.VMEM((rows, out), jnp.bfloat16),
        pltpu.VMEM(projected.shape, jnp.float32),
        pltpu.VMEM(params.shape, jnp.float32),
        pltpu.VMEM((2, out), jnp.float32),
    ]
    sems = [pltpu.SemaphoreType.DMA((3 + parts,)), pltpu.SemaphoreType.DMA((parts,))]
    operands = [x, projected, params, received]
    if follow is not None:
        mid = follow[0].shape[2]
        outs.append((jax.ShapeDtypeStruct((2, out), jnp.float32), True))
        outs.append((jax.ShapeDtypeStruct((members, 2, mid), jnp.float32), True))
        scratch += [pltpu.VMEM((out, mid), jnp.bfloat16), pltpu.VMEM((2, mid), jnp.float32)]
        sems.insert(1, pltpu.SemaphoreType.DMA((2,)))
        operands += list(follow)
        inside = ()
    else:
        outs += [(jax.ShapeDtypeStruct((LAYERS, out), jnp.float32), True)] * 2
        scratch.insert(0, pltpu.VMEM((2, out), jnp.float32))
        operands.append(earlier)
        inside = (4,)
    return call(
        functools.partial(
            output_kernel, layer=layer, parts=parts, row_count=row_count, follow=follow is not None
        ),
        "block_output", inside, outs, scratch + sems, 24, *operands,
    )


def exchange(stats):
    sums = lax.all_to_all(stats, "row", split_axis=0, concat_axis=0, tiled=True)
    total = jnp.sum(sums, axis=0)
    copies = jnp.broadcast_to(total[None], (lax.axis_size("col"),) + total.shape)
    return jnp.sum(lax.all_to_all(copies, "col", split_axis=0, concat_axis=0, tiled=True), axis=0)


def per_device(
    images, expand_weight, depth_kernel, squeeze_weight, squeeze_bias, excite_weight, excite_bias,
    project_weight, mid_gain, mid_bias, out_gain, out_bias, mid_mean, mid_var, out_mean, out_var,
):
    batch, side, _, out = images.shape
    mid = expand_weight.shape[2]
    members = lax.axis_size("row")
    row_count = float(batch * side * side * members * lax.axis_size("col"))
    spare = -mid % LANE
    widen = lambda a: jnp.pad(a, [(0, 0)] * (a.ndim - 1) + [(0, spare)])
    current = jnp.transpose(images, (1, 2, 0, 3)).reshape(side * side * batch, out)
    stats = moments_call(current, expand_weight, mid_mean, 0, members)
    params = jnp.stack([mid_mean, mid_var, mid_gain, mid_bias], axis=2)
    params = widen(params.reshape(LAYERS * 2 * 4, mid))
    out_params = jnp.stack([out_mean, out_var, out_gain, out_bias], axis=1).reshape(LAYERS * 4, out)
    mid_new, out_new = [], []
    for layer in range(LAYERS):
        spread, stats, first_new = depth_call(
            current, expand_weight, depth_kernel, params, exchange(stats), members, layer, side, row_count
        )
        projected, stats, second_new = lift_call(
            spread, params, squeeze_weight, squeeze_bias, excite_weight, excite_bias,
            project_weight, out_mean, exchange(stats), members, layer, row_count,
        )
        received = exchange(stats)
        if layer + 1 < LAYERS:
            current, third_new, stats = output_call(
                current, projected, out_params, received, members, layer, row_count, (expand_weight, mid_mean)
            )
            out_new.append(third_new)
        else:
            earlier = jnp.stack(out_new, axis=1)
            current, out_mean_new, out_var_new = output_call(
                current, projected, out_params, received, members, layer, row_count, None, earlier
            )
        mid_new.append(jnp.stack([first_new, second_new]))
    mid_new = jnp.stack(mid_new)
    block_output = jnp.transpose(current.reshape(side, side, batch, out), (2, 0, 1, 3))
    return block_output, mid_new[:, :, 0], mid_new[:, :, 1], out_mean_new, out_var_new


def solution(mesh):
    split = P(("row", "col"), None, None, None)
    return jax.shard_map(
        per_device, mesh=mesh, in_specs=(split,) + (P(),) * 15, out_specs=(split, P(), P(), P(), P()), check_vma=False
    )
```
